32 devices in a mesh: fsdp: 8 (over z, y), dp: 4 (over x, core).
Axes of the slice: x: 2, y: 2, z: 4, core: 2. Of those that a mesh axis runs over, the one named last changes fastest.
Arguments:
- tokens: bfloat16 [32, 128, 3584], P(('fsdp', 'dp')), may hold values from -6 to 6
- lengths: int32 [32], P(('fsdp', 'dp')), may hold values from 32 to 128
- partner: int32 [32], replicated, may hold values from 0 to 31, as said below
- pair_weight: float32 [32], P(('fsdp', 'dp')), may hold values from 0.25 to 27
- norm_gain: float32 [3584], replicated, may hold values from 0.5 to 1.5
- qkv_weight: bfloat16 [3584, 4608], P('fsdp'), may hold values from -0.09375 to 0.09375
- qkv_bias: float32 [4608], replicated, may hold values from -40 to 40
- out_weight: bfloat16 [3584, 3584], P(None, 'fsdp'), may hold values from -0.09375 to 0.09375
- final_gain: float32 [3584], replicated, may hold values from 0.5 to 1.5
- value_head: float32 [3584], replicated, may hold values from -0.09375 to 0.09375
Outputs:
- hidden: bfloat16 [32, 128, 3584], P(('fsdp', 'dp'))
- margins: float32 [32], P(('fsdp', 'dp'))
- loss: float32 [], replicated
The draws below stay inside these ranges and needn't reach their ends.
Inputs may be any that keep to these rules, and one draw needn't show every extreme that they name: partner[partner[i]] = i and partner[i] != i.
All inputs are finite; a program needn't handle non-finite values.
Results may differ from the reference program's by a relative error of at most 0.013.
The reference program's roundings to bfloat16 on the way count: a program that leaves them out, or rounds other values in their place, can miss the bound.
Values may be sent and summed in bfloat16 or wider, within the bound.
No kernel may reach another device: no remote copies, remote signals or barrier semaphores. Data moves between devices by JAX's collectives and lax.ppermute only.
A program may use at most 128 MiB of HBM per device.

```python
import jax
import jax.numpy as jnp
from jax import lax

D = 3584
QUERY_HEADS = 28
KEY_VALUE_HEADS = 4
HEAD_SIZE = 128
SEQUENCE_TOKENS = 128
QUERY_FEATURES = 3584
KEY_FEATURES = 512
QKV = 4608
SEQS = 32


def draw_partner(key, part):
    half = SEQS // 2
    anchor = jax.random.randint(jax.random.fold_in(key, 31), (), 0, half - 2).astype(jnp.int32)
    ranks = jax.random.permutation(jax.random.fold_in(key, 32), SEQS).astype(jnp.int32)
    index = jnp.arange(SEQS, dtype=jnp.int32)
    far_end = anchor + half
    near_one = anchor + 1
    near_two = anchor + 2
    used = (index == anchor) | (index == far_end) | (index == near_one) | (index == near_two)
    sort_key = jnp.where(used, SEQS + ranks, ranks)
    order = jnp.argsort(sort_key, stable=True).astype(jnp.int32)
    rest = order[:SEQS - 4]
    first = rest[0::2]
    second = rest[1::2]
    result = jnp.zeros((SEQS,), jnp.int32)
    result = result.at[first].set(second)
    result = result.at[second].set(first)
    result = result.at[anchor].set(far_end)
    result = result.at[far_end].set(anchor)
    result = result.at[near_one].set(near_two)
    result = result.at[near_two].set(near_one)
    return result


def draw_pair_weight(key, part):
    position = jnp.arange(SEQS, dtype=jnp.float32) / jnp.float32(max(SEQS - 1, 1))
    rising = jnp.exp(position * jnp.log(jnp.float32(9.0)))
    rough = jax.random.uniform(jax.random.fold_in(key, 22), (SEQS,), jnp.float32, 0.5, 1.5)
    return jnp.clip(rising * rough, 0.25, 27.0).astype(jnp.float32)


def draw_qkv_bias(key, part):
    key_three = jax.random.fold_in(key, 13)
    result = 0.5 * jax.random.normal(key_three, (QKV,), jnp.float32)
    return jnp.clip(result, -40.0, 40.0).astype(jnp.float32)


def plant(entries, stream_key, smallest, top_value):
    place = [jax.random.randint(jax.random.fold_in(stream_key, axis), (), 0, length) for axis, length in enumerate(entries.shape)]
    main_axis = entries.shape.index(max(entries.shape))
    beside = place[:main_axis] + [(place[main_axis] + 1) % entries.shape[main_axis]] + place[main_axis + 1:]
    return entries.at[tuple(place)].set(smallest).at[tuple(beside)].set(top_value)


def level_of(rng, dims, shards, low, high):
    def one(dim, parts):
        steps = jax.random.uniform(jax.random.fold_in(jax.random.fold_in(rng, 6), dim), (parts,), jnp.float32, low / len(shards), high / len(shards))
        return jnp.repeat(jnp.exp(steps), dims[dim] // parts).reshape((-1,) + (1,) * (len(dims) - dim - 1))

    level = one(*shards[0])
    for cut in shards[1:]:
        level = level * one(*cut)
    return level


def bell_draw(key, dims, scale, limit, split=(), kind=jnp.bfloat16):
    values = jax.random.normal(key, dims, jnp.float32) * scale
    if len(split) > 0:
        values = level_of(key, dims, split, -0.22, 0.18) * values
    return jnp.clip(values, min=-limit, max=limit).astype(kind)


def setup_inputs(seed: int = 0) -> dict:
    streams_of = jax.random.split(jax.random.key(seed), 11)
    return {
        "tokens": bell_draw(streams_of[0], (SEQS, SEQUENCE_TOKENS, D), 1.0, 6.0, ((0, 32),)),
        "lengths": plant(jax.random.randint(streams_of[1], (SEQS,), SEQUENCE_TOKENS // 4, SEQUENCE_TOKENS + 1), jax.random.fold_in(streams_of[1], 1), SEQUENCE_TOKENS // 4, SEQUENCE_TOKENS).astype(jnp.int32),
        "partner": draw_partner(jax.random.fold_in(streams_of[10], 71), 0),
        "pair_weight": draw_pair_weight(jax.random.fold_in(streams_of[10], 71), 0),
        "norm_gain": jnp.clip(1.0 + 0.1 * jax.random.normal(streams_of[4], (D,), jnp.float32), 0.5, 1.5),
        "qkv_weight": bell_draw(streams_of[5], (D, QKV), D ** -0.5, 0.09375, ((0, 8),)),
        "qkv_bias": draw_qkv_bias(jax.random.fold_in(streams_of[10], 71), 0),
        "out_weight": bell_draw(streams_of[7], (QUERY_FEATURES, D), QUERY_FEATURES ** -0.5, 0.09375, ((1, 8),)),
        "final_gain": jnp.clip(1.0 + 0.1 * jax.random.normal(streams_of[8], (D,), jnp.float32), 0.5, 1.5),
        "value_head": bell_draw(streams_of[9], (D,), D ** -0.5, 0.09375, (), jnp.float32),
    }


def rms_scale(value_rows, gain):
    return value_rows * lax.rsqrt(lax.optimization_barrier(jnp.mean(value_rows * value_rows, axis=-1, keepdims=True)) + 1e-06) * gain

def apply_rotary(heads):
    half = HEAD_SIZE // 2
    positions = jnp.arange(SEQUENCE_TOKENS, dtype=jnp.float32)
    freqs = jnp.exp(-(2.0 * jnp.arange(half, dtype=jnp.float32) / HEAD_SIZE) * jnp.log(jnp.float32(1000000.0)))
    angles = positions[:, None] * freqs[None, :]
    cosine = jnp.cos(angles)
    sine = jnp.sin(angles)
    first = heads[..., :half]
    second = heads[..., half:]
    return jnp.concatenate([first * cosine - second * sine, second * cosine + first * sine], axis=-1)

def one_sequence(sequence, length, norm_gain, qkv_weight, qkv_bias, out_weight, final_gain, value_head):
    normed = rms_scale(sequence.astype(jnp.float32), norm_gain).astype(jnp.bfloat16)
    query_key_value = jnp.dot(normed, qkv_weight, preferred_element_type=jnp.float32) + qkv_bias
    query_rows = query_key_value[:, :QUERY_FEATURES].reshape(SEQUENCE_TOKENS, QUERY_HEADS, HEAD_SIZE).transpose(1, 0, 2)
    key_rows = query_key_value[:, QUERY_FEATURES:QUERY_FEATURES + KEY_FEATURES].reshape(SEQUENCE_TOKENS, KEY_VALUE_HEADS, HEAD_SIZE).transpose(1, 0, 2)
    value_rows = query_key_value[:, QUERY_FEATURES + KEY_FEATURES:].reshape(SEQUENCE_TOKENS, KEY_VALUE_HEADS, HEAD_SIZE).transpose(1, 0, 2).astype(jnp.bfloat16)
    query_rows = apply_rotary(query_rows).astype(jnp.bfloat16).reshape(KEY_VALUE_HEADS, QUERY_HEADS // KEY_VALUE_HEADS, SEQUENCE_TOKENS, HEAD_SIZE)
    key_rows = apply_rotary(key_rows).astype(jnp.bfloat16)
    scores = jnp.einsum('gqtd,gsd->gqts', query_rows.astype(jnp.float32), key_rows.astype(jnp.float32)) / jnp.sqrt(jnp.float32(HEAD_SIZE))
    rows = jnp.arange(SEQUENCE_TOKENS, dtype=jnp.int32)
    allowed = (rows[None, :] <= rows[:, None]) & (rows[None, :] < length)
    scores = jnp.where(allowed, scores, jnp.float32(-1e+30))
    top = lax.optimization_barrier(jnp.max(scores, axis=-1, keepdims=True))
    expd = jnp.exp(scores - top)
    probs = (expd / lax.optimization_barrier(jnp.sum(expd, axis=-1, keepdims=True))).astype(jnp.bfloat16)
    attn = jnp.einsum('gqts,gsd->gqtd', probs.astype(jnp.float32), value_rows.astype(jnp.float32))
    attn = attn.reshape(QUERY_HEADS, SEQUENCE_TOKENS, HEAD_SIZE).transpose(1, 0, 2).reshape(SEQUENCE_TOKENS, QUERY_FEATURES).astype(jnp.bfloat16)
    hidden = (sequence.astype(jnp.float32) + jnp.dot(attn, out_weight, preferred_element_type=jnp.float32)).astype(jnp.bfloat16)
    last = lax.dynamic_slice_in_dim(hidden, (length - 1).astype(jnp.int32), 1, 0)[0].astype(jnp.float32)
    score = jnp.sum(rms_scale(last, final_gain) * value_head)
    return (hidden, score)

def reference(tokens, lengths, partner, pair_weight, norm_gain, qkv_weight, qkv_bias, out_weight, final_gain, value_head):

    def step(item):
        return one_sequence(item[0], item[1], norm_gain, qkv_weight, qkv_bias, out_weight, final_gain, value_head)
    hidden, scores = lax.map(step, (tokens, lengths))
    other = scores[partner]
    index = jnp.arange(SEQS, dtype=jnp.int32)
    margins = jnp.where(index < partner, scores - other, other - scores)
    loss = jnp.sum(pair_weight * jax.nn.softplus(-margins)) / SEQS
    return (hidden, margins, loss)
```

```python
import jax
import jax.numpy as jnp
from jax import lax
from jax.experimental import pallas as pl
from jax.experimental.pallas import tpu as pltpu
from jax.sharding import PartitionSpec as P

QUERY_HEADS = 28
KEY_VALUE_HEADS = 4
HEAD_SIZE = 128
QUERY_FEATURES = 3584
KEY_FEATURES = 512
AXES = ("fsdp", "dp")


def rms_scale(value_rows, gain):
    return (
        value_rows
        * lax.rsqrt(jnp.mean(value_rows * value_rows, axis=-1, keepdims=True) + 1e-06)
        * gain
    )


def rotary_tables(length_rows):
    half = HEAD_SIZE // 2
    positions = jnp.arange(length_rows, dtype=jnp.float32)
    freqs = jnp.exp(
        -(2.0 * jnp.arange(half, dtype=jnp.float32) / HEAD_SIZE) * jnp.log(jnp.float32(1000000.0))
    )
    angles = positions[:, None] * freqs[None, :]
    cosine = jnp.cos(angles)
    sine = jnp.sin(angles)
    return (
        jnp.concatenate([cosine, cosine], axis=-1),
        jnp.concatenate([-sine, sine], axis=-1),
    )


def attention_kernel(query_heads, lengths_ref, acc_ref, bias_ref, cos_ref, sin_ref, out_ref):
    length = lengths_ref[pl.program_id(0)]
    rows = acc_ref.shape[0]
    cosine = cos_ref[...]
    sine = sin_ref[...]

    def head(index):
        cols = pl.ds(index * HEAD_SIZE, HEAD_SIZE)
        return acc_ref[:, cols] + bias_ref[:, cols]

    def rotate(values):
        return (
            values * cosine + pltpu.roll(values, HEAD_SIZE // 2, 1) * sine
        ).astype(jnp.bfloat16)

    key_rows = rotate(head(query_heads))
    value_rows = head(query_heads + 1).astype(jnp.bfloat16)
    row = lax.broadcasted_iota(jnp.int32, (rows, rows), 0)
    col = lax.broadcasted_iota(jnp.int32, (rows, rows), 1)
    allowed = (col <= row) & (col < length)
    scale = jnp.sqrt(jnp.float32(HEAD_SIZE))
    for index in range(query_heads):
        scores = (
            lax.dot_general(
                rotate(head(index)),
                key_rows,
                (((1,), (1,)), ((), ())),
                preferred_element_type=jnp.float32,
            )
            / scale
        )
        scores = jnp.where(allowed, scores, jnp.float32(-1e30))
        expd = jnp.exp(scores - jnp.max(scores, axis=-1, keepdims=True))
        probs = (expd / jnp.sum(expd, axis=-1, keepdims=True)).astype(jnp.bfloat16)
        mixed = jnp.dot(probs, value_rows, preferred_element_type=jnp.float32)
        out_ref[:, pl.ds(index * HEAD_SIZE, HEAD_SIZE)] = mixed.astype(jnp.bfloat16)


def attend(acc, bias_cols, tables, group_lengths, query_heads, length_rows):
    total_rows, width = acc.shape
    seq_count = total_rows // length_rows
    query_cols = query_heads * HEAD_SIZE

    def kernel(*refs):
        attention_kernel(query_heads, *refs)

    return pl.pallas_call(
        kernel,
        name="attention",
        out_shape=jax.ShapeDtypeStruct((total_rows, query_cols), jnp.bfloat16),
        grid=(seq_count,),
        in_specs=[
            pl.BlockSpec(memory_space=pltpu.SMEM),
            pl.BlockSpec((length_rows, width), lambda i: (i, 0)),
            pl.BlockSpec((1, width), lambda i: (0, 0)),
            pl.BlockSpec((length_rows, HEAD_SIZE), lambda i: (0, 0)),
            pl.BlockSpec((length_rows, HEAD_SIZE), lambda i: (0, 0)),
        ],
        out_specs=pl.BlockSpec((length_rows, query_cols), lambda i: (i, 0)),
        cost_estimate=pl.CostEstimate(
            flops=4 * seq_count * query_heads * length_rows * length_rows * HEAD_SIZE * 8,
            bytes_accessed=acc.size * 4 + total_rows * query_cols * 2,
            transcendentals=seq_count * query_heads * length_rows * length_rows,
        ),
    )(group_lengths, acc, bias_cols.reshape(1, width), *tables)


def solution(mesh):
    fsdp_size = mesh.shape["fsdp"]
    dp_size = mesh.shape["dp"]
    planes = fsdp_size // 2
    ranks = dp_size
    query_heads = QUERY_HEADS // ranks
    key_value_heads = KEY_VALUE_HEADS // ranks
    query_cols = query_heads * HEAD_SIZE
    key_cols = key_value_heads * HEAD_SIZE

    def route(move):
        pairs = []
        for f in range(fsdp_size):
            for d in range(dp_size):
                target = move(f // 2, f % 2, d // 2, d % 2)
                if target is not None:
                    z, y, x, c = target
                    pairs.append((f * dp_size + d, (z * 2 + y) * dp_size + x * 2 + c))
        return pairs

    def send(array, move):
        return lax.ppermute(array, AXES, route(move))

    def to_y(z, y, x, c):
        return (z, 1 - y, x, c)

    def to_x(z, y, x, c):
        return (z, y, x ^ 1, c)

    def to_xy(z, y, x, c):
        return (z, 1 - y, x ^ 1, c)

    def to_core(z, y, x, c):
        return (z, y, x, 1 - c)

    def hop_y(z, y, x, c):
        return (z, 1 - y, x, 1 - c) if c != y else None

    def upward(step):
        return lambda z, y, x, c: (z + 1, y, x, c) if z >= step - 1 and z + 1 < planes else None

    def downward(step):
        return lambda z, y, x, c: (z - 1, y, x, c) if z + step <= planes and z >= 1 else None

    def gather_ranks(array):
        half = array.shape[0] // 2
        by_y = send(array, to_y)
        by_x = send(array, to_x)
        far = jnp.concatenate([send(by_x[:half], to_y), send(by_y[half:], to_x)], axis=0)
        return [array, by_y, by_x, far]

    def per_device(
        tokens,
        lengths,
        partner,
        pair_weight,
        norm_gain,
        qkv_weight,
        qkv_bias,
        out_weight,
        final_gain,
        value_head,
    ):
        f = lax.axis_index("fsdp")
        d = lax.axis_index("dp")
        z, y, x, c = f // 2, f % 2, d // 2, d % 2
        g = x * 2 + y
        sequence = tokens[0]
        length = lengths[0]
        length_rows, width = sequence.shape
        shard_rows = qkv_weight.shape[0]

        def group_slices(array, group, dim):
            return jnp.concatenate(
                [
                    lax.dynamic_slice_in_dim(array, group * query_cols, query_cols, dim),
                    lax.dynamic_slice_in_dim(
                        array, QUERY_FEATURES + group * key_cols, key_cols, dim
                    ),
                    lax.dynamic_slice_in_dim(
                        array, QUERY_FEATURES + KEY_FEATURES + group * key_cols, key_cols, dim
                    ),
                ],
                axis=dim,
            )

        def spread(first, idle):
            found = [(z, first)]
            up = down = first
            for step in range(1, planes):
                up = send(up, upward(step))
                down = send(down, downward(step))
                if 2 * step < planes:
                    found.append((jnp.where(z >= step, z - step, z - step + planes), up))
                    found.append(
                        (jnp.where(z + step < planes, z + step, z + step - planes), down)
                    )
                else:
                    from_low = z >= step
                    from_high = z + step < planes
                    found.append(
                        (
                            jnp.where(from_low, z - step, jnp.where(from_high, z + step, z)),
                            jnp.where(from_low, up, jnp.where(from_high, down, idle)),
                        )
                    )
            return found

        near = c == y
        cut = group_slices(qkv_weight, jnp.where(near, g, g ^ 1), 1)
        block = jnp.where(near, cut, send(cut, hop_y))
        qkv_blocks = spread(block, jnp.bfloat16(0))

        by_rank = jnp.stack(gather_ranks(sequence))
        length_by_rank = jnp.stack(
            [lengths, send(lengths, to_y), send(lengths, to_x), send(lengths, to_xy)]
        )[:, 0]
        order = [g ^ j for j in range(ranks)]
        group_tokens = jnp.stack(
            [lax.dynamic_index_in_dim(by_rank, j, 0, False) for j in order]
        )
        group_lengths = jnp.stack(
            [lax.dynamic_index_in_dim(length_by_rank, j, 0, False) for j in order]
        )
        normed = rms_scale(group_tokens.astype(jnp.float32), norm_gain).astype(jnp.bfloat16)
        rows = ranks * length_rows
        normed = normed.reshape(rows, fsdp_size, shard_rows).transpose(1, 0, 2)
        acc = None
        for plane, own in qkv_blocks:
            other = send(own, to_core)
            for core, weights in ((c, own), (1 - c, other)):
                part = jnp.dot(
                    lax.dynamic_index_in_dim(normed, plane * 2 + core, 0, False),
                    weights,
                    preferred_element_type=jnp.float32,
                )
                acc = part if acc is None else acc + part

        attn = attend(
            acc,
            group_slices(qkv_bias, g, 0),
            rotary_tables(length_rows),
            group_lengths,
            query_heads,
            length_rows,
        )
        attn_parts = gather_ranks(attn)

        out_cols = out_weight.shape[1] // ranks
        cut = lax.dynamic_slice_in_dim(out_weight.T, d * out_cols, out_cols, 0)
        first = jnp.stack(
            [
                lax.dynamic_slice_in_dim(cut, (g ^ j) * query_cols, query_cols, 1)
                for j in range(ranks)
            ]
        )
        out_full = jnp.zeros((ranks, planes, 2, out_cols, query_cols), jnp.bfloat16)
        for plane, own in spread(first, first):
            other = send(own, to_core)
            for core, weights in ((c, own), (1 - c, other)):
                out_full = lax.dynamic_update_slice(
                    out_full, weights[:, None, None], (0, plane, core, 0, 0)
                )
        projected = None
        for j in range(ranks):
            part = lax.dot_general(
                attn_parts[j],
                out_full[j].reshape(planes * 2 * out_cols, query_cols),
                (((1,), (1,)), ((), ())),
                preferred_element_type=jnp.float32,
            )
            projected = part if projected is None else projected + part
        projected = projected.astype(jnp.bfloat16).reshape(ranks, length_rows, -1)

        def rows_of(j):
            return lax.dynamic_index_in_dim(projected, g ^ j, 0, False)

        pieces = jnp.stack(
            [rows_of(0), send(rows_of(1), to_y), send(rows_of(2), to_x), send(rows_of(3), to_xy)]
        )
        ordered = jnp.stack(
            [
                lax.dynamic_index_in_dim(
                    pieces, g ^ ((r % 2) * 2 + r // 2), 0, False
                ).reshape(length_rows, planes, 2 * out_cols)
                for r in range(ranks)
            ],
            axis=2,
        ).reshape(length_rows, width)
        hidden = (sequence.astype(jnp.float32) + ordered.astype(jnp.float32)).astype(jnp.bfloat16)
        last = lax.dynamic_slice_in_dim(hidden, length - 1, 1, 0)[0].astype(jnp.float32)
        score = jnp.sum(rms_scale(last, final_gain) * value_head)

        both = jnp.stack([score, pair_weight[0]]).reshape(1, 2)
        near_dp = [both]
        for j in range(1, dp_size):
            pairs = [
                (a * dp_size + b, a * dp_size + (b + j) % dp_size)
                for a in range(fsdp_size)
                for b in range(dp_size)
            ]
            near_dp.append(lax.ppermute(both, AXES, pairs))
        group = jnp.concatenate(near_dp, axis=0)
        all_groups = [group]
        for j in range(1, fsdp_size):
            pairs = [
                (a * dp_size + b, ((a + j) % fsdp_size) * dp_size + b)
                for a in range(fsdp_size)
                for b in range(dp_size)
            ]
            all_groups.append(lax.ppermute(group, AXES, pairs))
        gathered = jnp.stack(all_groups)
        from_f = lax.rem(f - jnp.arange(fsdp_size, dtype=jnp.int32) + fsdp_size, fsdp_size)
        from_d = lax.rem(d - jnp.arange(dp_size, dtype=jnp.int32) + dp_size, dp_size)
        ids = (from_f[:, None] * dp_size + from_d[None, :]).reshape(-1)
        scores = gathered[..., 0].reshape(-1)
        weights = gathered[..., 1].reshape(-1)
        total_seqs = fsdp_size * dp_size
        index_all = jnp.arange(total_seqs, dtype=jnp.int32)
        mine = f * dp_size + d
        everyone = jnp.sum(
            jnp.where(ids[None, :] == index_all[:, None], scores[None, :], 0.0), axis=1
        )
        weights_all = jnp.sum(
            jnp.where(ids[None, :] == index_all[:, None], weights[None, :], 0.0), axis=1
        )
        matches = partner[:, None] == index_all[None, :]
        others_all = jnp.sum(jnp.where(matches, everyone[None, :], jnp.float32(0.0)), axis=1)
        margins_all = jnp.where(index_all < partner, everyone - others_all, others_all - everyone)
        margin = jnp.sum(jnp.where(index_all == mine, margins_all, 0.0))
        loss = jnp.sum(weights_all * jax.nn.softplus(-margins_all)) / total_seqs
        return (hidden[None], margin.reshape(1), loss)

    return jax.shard_map(
        per_device,
        mesh=mesh,
        in_specs=(
            P(("fsdp", "dp"), None, None),
            P(("fsdp", "dp")),
            P(),
            P(("fsdp", "dp")),
            P(),
            P("fsdp", None),
            P(),
            P(None, "fsdp"),
            P(),
            P(),
        ),
        out_specs=(P(("fsdp", "dp"), None, None), P(("fsdp", "dp")), P()),
        check_vma=False,
    )
```

```python
import jax
import jax.numpy as jnp
from jax import lax
from jax.experimental import pallas as pl
from jax.experimental.pallas import tpu as pltpu
from jax.sharding import PartitionSpec as P

QUERY_HEADS = 28
KEY_VALUE_HEADS = 4
HEAD_SIZE = 128
QUERY_FEATURES = 3584
KEY_FEATURES = 512
AXES = ("fsdp", "dp")


def rms_scale(value_rows, gain):
    return (
        value_rows
        * lax.rsqrt(jnp.mean(value_rows * value_rows, axis=-1, keepdims=True) + 1e-06)
        * gain
    )


def rotary_tables(length_rows):
    half = HEAD_SIZE // 2
    positions = jnp.arange(length_rows, dtype=jnp.float32)
    freqs = jnp.exp(
        -(2.0 * jnp.arange(half, dtype=jnp.float32) / HEAD_SIZE) * jnp.log(jnp.float32(1000000.0))
    )
    angles = positions[:, None] * freqs[None, :]
    cosine = jnp.cos(angles)
    sine = jnp.sin(angles)
    return (
        jnp.concatenate([cosine, cosine], axis=-1),
        jnp.concatenate([-sine, sine], axis=-1),
    )


def attention_kernel(
    query_heads, order_ref, lengths_ref, acc_ref, bias_ref, cos_ref, sin_ref, out_ref
):
    del order_ref
    length = lengths_ref[pl.program_id(0)]
    rows = acc_ref.shape[0]
    cosine = cos_ref[...]
    sine = sin_ref[...]

    def head(index):
        cols = pl.ds(index * HEAD_SIZE, HEAD_SIZE)
        return acc_ref[:, cols] + bias_ref[:, cols]

    def rotate(values):
        return (
            values * cosine + pltpu.roll(values, HEAD_SIZE // 2, 1) * sine
        ).astype(jnp.bfloat16)

    key_rows = rotate(head(query_heads))
    value_rows = head(query_heads + 1).astype(jnp.bfloat16)
    row = lax.broadcasted_iota(jnp.int32, (rows, rows), 0)
    col = lax.broadcasted_iota(jnp.int32, (rows, rows), 1)
    allowed = (col <= row) & (col < length)
    scale = 1.0 / jnp.sqrt(jnp.float32(HEAD_SIZE))
    for index in range(query_heads):
        scores = (
            lax.dot_general(
                rotate(head(index)),
                key_rows,
                (((1,), (1,)), ((), ())),
                preferred_element_type=jnp.float32,
            )
            * scale
        )
        scores = jnp.where(allowed, scores, jnp.float32(-1e30))
        expd = jnp.exp(scores - jnp.max(scores, axis=-1, keepdims=True))
        inverse = 1.0 / jnp.sum(expd, axis=-1, keepdims=True)
        probs = (expd * inverse).astype(jnp.bfloat16)
        mixed = jnp.dot(probs, value_rows, preferred_element_type=jnp.float32)
        out_ref[:, pl.ds(index * HEAD_SIZE, HEAD_SIZE)] = mixed.astype(jnp.bfloat16)


def attend(acc, bias_cols, tables, order, group_lengths, query_heads, length_rows):
    total_rows, width = acc.shape
    seq_count = total_rows // length_rows
    query_cols = query_heads * HEAD_SIZE

    def kernel(*refs):
        attention_kernel(query_heads, *refs)

    return pl.pallas_call(
        kernel,
        name="attention",
        out_shape=jax.ShapeDtypeStruct((total_rows, query_cols), jnp.bfloat16),
        grid_spec=pltpu.PrefetchScalarGridSpec(
            num_scalar_prefetch=2,
            grid=(seq_count,),
            in_specs=[
                pl.BlockSpec((length_rows, width), lambda i, order, lengths: (i, 0)),
                pl.BlockSpec((1, width), lambda i, order, lengths: (0, 0)),
                pl.BlockSpec((length_rows, HEAD_SIZE), lambda i, order, lengths: (0, 0)),
                pl.BlockSpec((length_rows, HEAD_SIZE), lambda i, order, lengths: (0, 0)),
            ],
            out_specs=pl.BlockSpec(
                (length_rows, query_cols), lambda i, order, lengths: (order[i], 0)
            ),
        ),
        cost_estimate=pl.CostEstimate(
            flops=32 * seq_count * query_heads * length_rows * length_rows * HEAD_SIZE,
            bytes_accessed=acc.size * 4 + total_rows * query_cols * 2,
            transcendentals=seq_count * query_heads * length_rows * length_rows,
        ),
    )(order, group_lengths, acc, bias_cols.reshape(1, width), *tables)


def norm_kernel(own_ref, by_y_ref, by_x_ref, far_a_ref, far_b_ref, gain_ref, out_ref):
    shards, _, shard_rows = out_ref.shape
    step = 16
    base = 0
    for source in (own_ref, by_y_ref, by_x_ref, far_a_ref, far_b_ref):

        def body(i, carry, source=source, base=base):
            start = pl.multiple_of(i * step, step)
            values = source[pl.ds(start, step), :].astype(jnp.float32)
            normed = rms_scale(values, gain_ref[...]).astype(jnp.bfloat16)
            target = pl.ds(pl.multiple_of(base + i * step, step), step)
            for s in range(shards):
                out_ref[s, target, :] = normed[:, s * shard_rows : (s + 1) * shard_rows]
            return carry

        lax.fori_loop(0, source.shape[0] // step, body, 0)
        base += source.shape[0]


def normalise(parts, gain, shards):
    rows = sum(part.shape[0] for part in parts)
    width = gain.shape[0]
    return pl.pallas_call(
        norm_kernel,
        name="normalise",
        out_shape=jax.ShapeDtypeStruct((shards, rows, width // shards), jnp.bfloat16),
        cost_estimate=pl.CostEstimate(
            flops=8 * rows * width, bytes_accessed=4 * rows * width, transcendentals=rows
        ),
    )(*parts, gain.reshape(1, width))


def project_kernel(ranks, core_ref, *refs):
    attn_refs, weight_refs, out_ref, full_ref = refs[:ranks], refs[ranks:-2], refs[-2], refs[-1]
    cols = weight_refs[0].shape[1]
    for block in range(out_ref.shape[0]):
        own_ref, other_ref = weight_refs[2 * block], weight_refs[2 * block + 1]

        @pl.when(core_ref[0] == 0)
        def _():
            full_ref[:, :cols, :] = own_ref[...]
            full_ref[:, cols:, :] = other_ref[...]

        @pl.when(core_ref[0] == 1)
        def _():
            full_ref[:, :cols, :] = other_ref[...]
            full_ref[:, cols:, :] = own_ref[...]

        total = None
        for j in range(ranks):
            part = lax.dot_general(
                attn_refs[j][...],
                full_ref[j],
                (((1,), (1,)), ((), ())),
                preferred_element_type=jnp.float32,
            )
            total = part if total is None else total + part
        out_ref[block] = total.astype(jnp.bfloat16)


def project(attn_parts, weights, core):
    ranks, cols, depth = weights[0].shape
    blocks = len(weights) // 2
    rows = attn_parts[0].shape[0]

    def kernel(*refs):
        project_kernel(ranks, *refs)

    return pl.pallas_call(
        kernel,
        name="project",
        out_shape=jax.ShapeDtypeStruct((blocks, rows, 2 * cols), jnp.bfloat16),
        in_specs=[pl.BlockSpec(memory_space=pltpu.SMEM)]
        + [pl.BlockSpec(memory_space=pltpu.VMEM)] * (ranks + len(weights)),
        scratch_shapes=[pltpu.VMEM((ranks, 2 * cols, depth), jnp.bfloat16)],
        cost_estimate=pl.CostEstimate(
            flops=2 * rows * ranks * depth * 2 * cols * blocks,
            bytes_accessed=2 * (rows * ranks * depth + 2 * blocks * ranks * cols * depth),
            transcendentals=0,
        ),
    )(core.reshape(1), *attn_parts, *weights)


def finish_kernel(ranks, place_ref, tokens_ref, gain_ref, head_ref, *refs):
    pieces, hidden_ref, score_ref = refs[:-2], refs[-2], refs[-1]
    flip_y = place_ref[0] == 1
    flip_x = place_ref[1] == 1
    length = place_ref[2]
    early = pieces[0].shape[0]
    rows, width = tokens_ref.shape
    planes = place_ref.shape[0] - 3
    wide = width // planes
    square = jnp.zeros((1, 1), jnp.float32)
    dotted = jnp.zeros((1, 1), jnp.float32)
    picked = lax.broadcasted_iota(jnp.int32, (rows, 1), 0) == length - 1
    gained = gain_ref[...] * head_ref[...]
    for plane in range(planes):
        slot = place_ref[3 + plane]

        def piece(j):
            value = pieces[2 * j][jnp.minimum(slot, early - 1)]
            late = pieces[2 * j + 1][0]
            return jnp.where(slot >= early, late, value).astype(jnp.float32)

        own, by_y, by_x, far = (piece(j) for j in range(ranks))
        y0x0, y1x0 = jnp.where(flip_y, by_y, own), jnp.where(flip_y, own, by_y)
        y0x1, y1x1 = jnp.where(flip_y, far, by_x), jnp.where(flip_y, by_x, far)
        ordered = [
            jnp.where(flip_x, y0x1, y0x0),
            jnp.where(flip_x, y0x0, y0x1),
            jnp.where(flip_x, y1x1, y1x0),
            jnp.where(flip_x, y1x0, y1x1),
        ]
        cols = slice(plane * wide, (plane + 1) * wide)
        hidden = (
            tokens_ref[:, cols].astype(jnp.float32) + jnp.concatenate(ordered, axis=1)
        ).astype(jnp.bfloat16)
        hidden_ref[:, cols] = hidden
        last = jnp.sum(jnp.where(picked, hidden.astype(jnp.float32), 0.0), axis=0, keepdims=True)
        square += jnp.sum(last * last, axis=1, keepdims=True)
        dotted += jnp.sum(last * gained[:, cols], axis=1, keepdims=True)
    score_ref[...] = jnp.broadcast_to(
        dotted * lax.rsqrt(square / width + 1e-06), score_ref.shape
    )


def finish(place, tokens, gain, head, pieces, ranks):
    rows, width = tokens.shape

    def kernel(*refs):
        finish_kernel(ranks, *refs)

    return pl.pallas_call(
        kernel,
        name="finish",
        out_shape=(
            jax.ShapeDtypeStruct((rows, width), jnp.bfloat16),
            jax.ShapeDtypeStruct((1, 128), jnp.float32),
        ),
        in_specs=[pl.BlockSpec(memory_space=pltpu.SMEM)]
        + [pl.BlockSpec(memory_space=pltpu.VMEM)] * (3 + len(pieces)),
        cost_estimate=pl.CostEstimate(
            flops=8 * rows * width, bytes_accessed=6 * rows * width, transcendentals=1
        ),
    )(place, tokens, gain.reshape(1, width), head.reshape(1, width), *pieces)


def solution(mesh):
    fsdp_size = mesh.shape["fsdp"]
    dp_size = mesh.shape["dp"]
    planes = fsdp_size // 2
    ranks = dp_size
    query_heads = QUERY_HEADS // ranks
    key_value_heads = KEY_VALUE_HEADS // ranks
    query_cols = query_heads * HEAD_SIZE
    key_cols = key_value_heads * HEAD_SIZE

    def route(move):
        pairs = []
        for f in range(fsdp_size):
            for d in range(dp_size):
                target = move(f // 2, f % 2, d // 2, d % 2)
                if target is not None:
                    z, y, x, c = target
                    pairs.append((f * dp_size + d, (z * 2 + y) * dp_size + x * 2 + c))
        return pairs

    def send(array, move):
        return lax.ppermute(array, AXES, route(move))

    def to_y(z, y, x, c):
        return (z, 1 - y, x, c)

    def to_x(z, y, x, c):
        return (z, y, x ^ 1, c)

    def to_xy(z, y, x, c):
        return (z, 1 - y, x ^ 1, c)

    def to_core(z, y, x, c):
        return (z, y, x, 1 - c)

    def hop_y(z, y, x, c):
        return (z, 1 - y, x, 1 - c) if c != y else None

    def along(shift, holds):
        def move(z, y, x, c):
            return (z + shift, y, x, c) if holds(z) and 0 <= z + shift < planes else None

        return move

    def crossed(move):
        def moved(z, y, x, c):
            target = move(z, y, x, c)
            if target is None or c == y:
                return target
            return (target[0], 1 - y, x, 1 - c)

        return moved

    def outward(step):
        def move(z, y, x, c):
            if z >= step - 1:
                return (z + 1, y, x, c) if z + 1 < planes else None
            if z + step <= planes:
                return (z - 1, y, x, c) if z >= 1 else None
            return None

        return move

    def gather_ranks(array):
        half = array.shape[0] // 2
        by_y = send(array, to_y)
        by_x = send(array, to_x)
        far = (send(by_x[:half], to_y), send(by_y[half:], to_x))
        return (array, by_y, by_x, *far)

    def per_device(
        tokens,
        lengths,
        partner,
        pair_weight,
        norm_gain,
        qkv_weight,
        qkv_bias,
        out_weight,
        final_gain,
        value_head,
    ):
        f = lax.axis_index("fsdp")
        d = lax.axis_index("dp")
        z, y, x, c = f // 2, f % 2, d // 2, d % 2
        g = x * 2 + y
        sequence = tokens[0]
        length = lengths[0]
        length_rows, width = sequence.shape
        shard_rows = qkv_weight.shape[0]

        def group_slices(array, group, dim):
            return jnp.concatenate(
                [
                    lax.dynamic_slice_in_dim(array, group * query_cols, query_cols, dim),
                    lax.dynamic_slice_in_dim(
                        array, QUERY_FEATURES + group * key_cols, key_cols, dim
                    ),
                    lax.dynamic_slice_in_dim(
                        array, QUERY_FEATURES + KEY_FEATURES + group * key_cols, key_cols, dim
                    ),
                ],
                axis=dim,
            )

        def spread(own, cut, first_move):
            found = [(z, own)]
            up = down = merged = None
            for step in range(1, planes):
                low, high = z >= step, z + step < planes
                below = jnp.where(low, z - step, -1)
                above = jnp.where(high, z + step, -1)
                if 2 * step <= planes:
                    go_up = along(1, lambda p, step=step: p >= step - 1)
                    go_down = along(-1, lambda p, step=step: p + step <= planes)
                    if step == 1:
                        up = send(cut, first_move(go_up))
                        down = send(cut, first_move(go_down))
                    else:
                        up, down = send(up, go_up), send(down, go_down)
                    if 2 * step < planes:
                        found += [(below, up), (above, down)]
                        continue
                    merged = jnp.where(low, up, down)
                else:
                    merged = send(merged, outward(step))
                found.append((jnp.where(low, below, above), merged))
            return found

        near = c == y
        cut = group_slices(qkv_weight, jnp.where(near, g, g ^ 1), 1)
        qkv_blocks = spread(jnp.where(near, cut, send(cut, hop_y)), cut, crossed)
        others = [send(own, to_core) for _, own in qkv_blocks]

        parts = gather_ranks(lax.optimization_barrier((sequence, cut))[0])
        group_lengths = jnp.stack(
            [lengths, send(lengths, to_y), send(lengths, to_x), send(lengths, to_xy)]
        )[:, 0]
        order = jnp.stack([g ^ j for j in range(ranks)])
        normed = normalise(parts, norm_gain, fsdp_size)
        acc = None
        for (plane, own), other in zip(qkv_blocks, others):
            for core, weights in ((c, own), (1 - c, other)):
                part = jnp.dot(
                    lax.dynamic_index_in_dim(
                        normed, jnp.maximum(plane, 0) * 2 + core, 0, False
                    ),
                    weights,
                    preferred_element_type=jnp.float32,
                )
                acc = part if acc is None else acc + part

        attn = attend(
            acc,
            group_slices(qkv_bias, g, 0),
            rotary_tables(length_rows),
            order,
            group_lengths,
            query_heads,
            length_rows,
        )
        attn_parts = gather_ranks(attn)
        attn_parts = attn_parts[:3] + (jnp.concatenate(attn_parts[3:], axis=0),)

        out_cols = out_weight.shape[1] // ranks
        cut = lax.dynamic_slice_in_dim(out_weight.T, d * out_cols, out_cols, 0)
        first = jnp.stack(
            [
                lax.dynamic_slice_in_dim(cut, (g ^ j) * query_cols, query_cols, 1)
                for j in range(ranks)
            ]
        )
        held = others[-2] if len(others) > 1 else others[0]
        first = lax.optimization_barrier((first, held))[0]
        out_blocks = spread(first, first, lambda move: move)
        pairs = [(own, send(own, to_core)) for _, own in out_blocks]
        early = project(attn_parts, [w for pair in pairs[:-1] for w in pair], c)
        late = project(attn_parts, list(pairs[-1]), c)

        def rows_of(array, j):
            start = (g ^ j) * length_rows
            return lax.dynamic_slice_in_dim(array, start, length_rows, 1)

        pieces = []
        for j, move in enumerate((None, to_y, to_x, to_xy)):
            for array in (early, late):
                piece = rows_of(array, j)
                pieces.append(piece if move is None else send(piece, move))
        slots = [
            sum(b * (plane == p).astype(jnp.int32) for b, (plane, _) in enumerate(out_blocks))
            for p in range(planes)
        ]
        place = jnp.stack([y, x, length, *slots]).astype(jnp.int32)
        hidden, scored = finish(place, sequence, final_gain, value_head, pieces, ranks)
        score = scored[0, 0]

        total_seqs = fsdp_size * dp_size
        index_all = jnp.arange(total_seqs, dtype=jnp.int32)
        mine = f * dp_size + d
        lane = lax.broadcasted_iota(jnp.int32, (total_seqs, 1, 128), 2)
        both = jnp.where(lane == 0, score, pair_weight[0])
        gathered = lax.all_to_all(both, AXES, 0, 0, tiled=True)
        everyone = gathered[:, 0, 0]
        weights_all = gathered[:, 0, 1]
        matches = partner[:, None] == index_all[None, :]
        others_all = jnp.sum(jnp.where(matches, everyone[None, :], jnp.float32(0.0)), axis=1)
        margins_all = jnp.where(index_all < partner, everyone - others_all, others_all - everyone)
        margin = jnp.sum(jnp.where(index_all == mine, margins_all, 0.0))
        loss = jnp.sum(weights_all * jax.nn.softplus(-margins_all)) / total_seqs
        return (hidden[None], margin.reshape(1), loss)

    return jax.shard_map(
        per_device,
        mesh=mesh,
        in_specs=(
            P(("fsdp", "dp"), None, None),
            P(("fsdp", "dp")),
            P(),
            P(("fsdp", "dp")),
            P(),
            P("fsdp", None),
            P(),
            P(None, "fsdp"),
            P(),
            P(),
        ),
        out_specs=(P(("fsdp", "dp"), None, None), P(("fsdp", "dp")), P()),
        check_vma=False,
    )
```

```python
import jax
import jax.numpy as jnp
from jax import lax
from jax.experimental import pallas as pl
from jax.experimental.pallas import tpu as pltpu
from jax.sharding import PartitionSpec as P


QUERY_HEADS = 28
KEY_VALUE_HEADS = 4
HEAD_SIZE = 128
QUERY_FEATURES = 3584
KEY_FEATURES = 512
AXES = ("fsdp", "dp")


def rms_scale(value_rows, gain):
    return (
        value_rows
        * lax.rsqrt(jnp.mean(value_rows * value_rows, axis=-1, keepdims=True) + 1e-06)
        * gain
    )


def rotary_tables(length_rows):
    half = HEAD_SIZE // 2
    positions = jnp.arange(length_rows, dtype=jnp.float32)
    freqs = jnp.exp(
        -(2.0 * jnp.arange(half, dtype=jnp.float32) / HEAD_SIZE) * jnp.log(jnp.float32(1000000.0))
    )
    angles = positions[:, None] * freqs[None, :]
    cosine = jnp.cos(angles)
    sine = jnp.sin(angles)
    return (
        jnp.concatenate([cosine, cosine], axis=-1),
        jnp.concatenate([-sine, sine], axis=-1),
    )


def attention_kernel(
    query_heads, lengths_ref, acc_ref, bias_ref, cos_ref, sin_ref, out_ref
):
    length = lengths_ref[pl.program_id(0)]
    rows = acc_ref.shape[0]
    cosine = cos_ref[...]
    sine = sin_ref[...]

    def head(index):
        cols = pl.ds(index * HEAD_SIZE, HEAD_SIZE)
        return acc_ref[:, cols] + bias_ref[:, cols]

    def rotate(values):
        return (
            values * cosine + pltpu.roll(values, HEAD_SIZE // 2, 1) * sine
        ).astype(jnp.bfloat16)

    key_rows = rotate(head(query_heads))
    value_rows = head(query_heads + 1).astype(jnp.bfloat16)
    row = lax.broadcasted_iota(jnp.int32, (rows, rows), 0)
    col = lax.broadcasted_iota(jnp.int32, (rows, rows), 1)
    allowed = (col <= row) & (col < length)
    scale = 1.0 / jnp.sqrt(jnp.float32(HEAD_SIZE))
    for index in range(query_heads):
        scores = (
            lax.dot_general(
                rotate(head(index)),
                key_rows,
                (((1,), (1,)), ((), ())),
                preferred_element_type=jnp.float32,
            )
            * scale
        )
        scores = jnp.where(allowed, scores, jnp.float32(-1e30))
        expd = jnp.exp(scores - jnp.max(scores, axis=-1, keepdims=True))
        inverse = 1.0 / jnp.sum(expd, axis=-1, keepdims=True)
        probs = (expd * inverse).astype(jnp.bfloat16)
        mixed = jnp.dot(probs, value_rows, preferred_element_type=jnp.float32)
        out_ref[:, pl.ds(index * HEAD_SIZE, HEAD_SIZE)] = mixed.astype(jnp.bfloat16)


def attend(acc, bias_cols, tables, group_lengths, query_heads, length_rows):
    total_rows, width = acc.shape
    seq_count = total_rows // length_rows
    query_cols = query_heads * HEAD_SIZE

    def kernel(*refs):
        attention_kernel(query_heads, *refs)

    return pl.pallas_call(
        kernel,
        name="attention",
        out_shape=jax.ShapeDtypeStruct((total_rows, query_cols), jnp.bfloat16),
        grid_spec=pltpu.PrefetchScalarGridSpec(
            num_scalar_prefetch=1,
            grid=(seq_count,),
            in_specs=[
                pl.BlockSpec((length_rows, width), lambda i, lengths: (i, 0)),
                pl.BlockSpec((1, width), lambda i, lengths: (0, 0)),
                pl.BlockSpec((length_rows, HEAD_SIZE), lambda i, lengths: (0, 0)),
                pl.BlockSpec((length_rows, HEAD_SIZE), lambda i, lengths: (0, 0)),
            ],
            out_specs=pl.BlockSpec((length_rows, query_cols), lambda i, lengths: (i, 0)),
        ),
        cost_estimate=pl.CostEstimate(
            flops=32 * seq_count * query_heads * length_rows * length_rows * HEAD_SIZE,
            bytes_accessed=acc.size * 4 + total_rows * query_cols * 2,
            transcendentals=seq_count * query_heads * length_rows * length_rows,
        ),
    )(group_lengths, acc, bias_cols.reshape(1, width), *tables)


def norm_kernel(own_ref, by_y_ref, by_x_ref, far_a_ref, far_b_ref, gain_ref, out_ref):
    shards, _, shard_rows = out_ref.shape
    step = 16
    base = 0
    for source in (own_ref, by_y_ref, by_x_ref, far_a_ref, far_b_ref):

        def body(i, carry, source=source, base=base):
            start = pl.multiple_of(i * step, step)
            values = source[pl.ds(start, step), :].astype(jnp.float32)
            normed = rms_scale(values, gain_ref[...]).astype(jnp.bfloat16)
            target = pl.ds(pl.multiple_of(base + i * step, step), step)
            for s in range(shards):
                out_ref[s, target, :] = normed[:, s * shard_rows : (s + 1) * shard_rows]
            return carry

        lax.fori_loop(0, source.shape[0] // step, body, 0)
        base += source.shape[0]


def normalise(parts, gain, shards):
    rows = sum(part.shape[0] for part in parts)
    width = gain.shape[0]
    return pl.pallas_call(
        norm_kernel,
        name="normalise",
        out_shape=jax.ShapeDtypeStruct((shards, rows, width // shards), jnp.bfloat16),
        cost_estimate=pl.CostEstimate(
            flops=8 * rows * width, bytes_accessed=4 * rows * width, transcendentals=rows
        ),
    )(*parts, gain.reshape(1, width))


def finish_kernel(groups, place_ref, tokens_ref, gain_ref, head_ref, *refs):
    pieces, hidden_ref, score_ref = refs[:-2], refs[-2], refs[-1]
    length = place_ref[0]
    rows, width = tokens_ref.shape
    planes = place_ref.shape[0] - 1
    wide = width // planes
    square = jnp.zeros((1, 1), jnp.float32)
    dotted = jnp.zeros((1, 1), jnp.float32)
    picked = lax.broadcasted_iota(jnp.int32, (rows, 1), 0) == length - 1
    gained = gain_ref[...] * head_ref[...]
    for plane in range(planes):
        slot = place_ref[1 + plane]
        cols = slice(plane * wide, (plane + 1) * wide)
        total = tokens_ref[:, cols].astype(jnp.float32)
        for first in range(0, len(pieces), groups):
            value = None
            base = 0
            for ref in pieces[first : first + groups]:
                count = ref.shape[0]
                part = ref[jnp.clip(slot - base, 0, count - 1)]
                value = part if value is None else jnp.where(slot >= base, part, value)
                base += count
            total += value.astype(jnp.float32)
        hidden = total.astype(jnp.bfloat16)
        hidden_ref[:, cols] = hidden
        last = jnp.sum(jnp.where(picked, hidden.astype(jnp.float32), 0.0), axis=0, keepdims=True)
        square += jnp.sum(last * last, axis=1, keepdims=True)
        dotted += jnp.sum(last * gained[:, cols], axis=1, keepdims=True)
    score_ref[...] = jnp.broadcast_to(
        dotted * lax.rsqrt(square / width + 1e-06), score_ref.shape
    )


def finish(place, tokens, gain, head, pieces, groups):
    rows, width = tokens.shape

    def kernel(*refs):
        finish_kernel(groups, *refs)

    return pl.pallas_call(
        kernel,
        name="finish",
        out_shape=(
            jax.ShapeDtypeStruct((rows, width), jnp.bfloat16),
            jax.ShapeDtypeStruct((1, 128), jnp.float32),
        ),
        in_specs=[pl.BlockSpec(memory_space=pltpu.SMEM)]
        + [pl.BlockSpec(memory_space=pltpu.VMEM)] * (3 + len(pieces)),
        cost_estimate=pl.CostEstimate(
            flops=8 * rows * width, bytes_accessed=6 * rows * width, transcendentals=1
        ),
    )(place, tokens, gain.reshape(1, width), head.reshape(1, width), *pieces)


def solution(mesh):
    fsdp_size = mesh.shape["fsdp"]
    dp_size = mesh.shape["dp"]
    planes = fsdp_size // 2
    ranks = dp_size
    query_heads = QUERY_HEADS // ranks
    key_value_heads = KEY_VALUE_HEADS // ranks
    query_cols = query_heads * HEAD_SIZE
    key_cols = key_value_heads * HEAD_SIZE

    def route(move):
        pairs = []
        for f in range(fsdp_size):
            for d in range(dp_size):
                target = move(f // 2, f % 2, d // 2, d % 2)
                if target is not None:
                    z, y, x, c = target
                    pairs.append((f * dp_size + d, (z * 2 + y) * dp_size + x * 2 + c))
        return pairs

    def send(array, move):
        return lax.ppermute(array, AXES, route(move))

    def to_y(z, y, x, c):
        return (z, 1 - y, x, c)

    def to_x(z, y, x, c):
        return (z, y, x ^ 1, c)

    def to_xy(z, y, x, c):
        return (z, 1 - y, x ^ 1, c)

    def to_core(z, y, x, c):
        return (z, y, x, 1 - c)

    def hop_y(z, y, x, c):
        return (z, 1 - y, x, 1 - c) if c != y else None

    def along(shift, holds):
        def move(z, y, x, c):
            return (z + shift, y, x, c) if holds(z) and 0 <= z + shift < planes else None

        return move

    def outward(step):
        def move(z, y, x, c):
            if z >= step - 1:
                return (z + 1, y, x, c) if z + 1 < planes else None
            if z + step <= planes:
                return (z - 1, y, x, c) if z >= 1 else None
            return None

        return move

    def whole(
        tokens,
        lengths,
        partner,
        pair_weight,
        norm_gain,
        qkv_weight,
        qkv_bias,
        out_weight,
        final_gain,
        value_head,
    ):
        f = lax.axis_index("fsdp")
        d = lax.axis_index("dp")
        z, y, x, c = f // 2, f % 2, d // 2, d % 2
        g = x * 2 + y
        sequence = tokens[0]
        length = lengths[0]
        length_rows, _ = sequence.shape

        def group_slices(array, group, dim):
            return jnp.concatenate(
                [
                    lax.dynamic_slice_in_dim(array, group * query_cols, query_cols, dim),
                    lax.dynamic_slice_in_dim(
                        array, QUERY_FEATURES + group * key_cols, key_cols, dim
                    ),
                    lax.dynamic_slice_in_dim(
                        array, QUERY_FEATURES + KEY_FEATURES + group * key_cols, key_cols, dim
                    ),
                ],
                axis=dim,
            )

        def spread(own, gate=None):
            found = [(z, own, 0)]
            up = down = merged = own
            for step in range(1, planes):
                low, high = z >= step, z + step < planes
                below = jnp.where(low, z - step, -1)
                above = jnp.where(high, z + step, -1)
                if 2 * step <= planes:
                    go_up = along(1, lambda p, step=step: p >= step - 1)
                    go_down = along(-1, lambda p, step=step: p + step <= planes)
                    up = send(up, go_up)
                    down = send(down, go_down)
                    if step == 1 and gate is not None:
                        up, down, _ = lax.optimization_barrier((up, down, gate))
                    if 2 * step < planes:
                        found += [(below, up, step), (above, down, step)]
                        continue
                    merged = jnp.where(low, up, down)
                else:
                    merged = send(merged, outward(step))
                found.append((jnp.where(low, below, above), merged, step))
            return found

        near = c == y

        def with_hop(cut):
            return jnp.where(near, cut, send(cut, hop_y))

        block = with_hop(group_slices(qkv_weight, jnp.where(near, g, g ^ 1), 1))
        qkv_blocks = spread(block)
        others = [send(own, to_core) for _, own, _ in qkv_blocks]

        half = length_rows // 2
        by_y = send(sequence, to_y)
        by_x = send(sequence, to_x)
        halves = by_x[:half], by_y[half:]
        far = [send(halves[0], to_y), send(halves[1], to_x)]
        normed = normalise([sequence, by_y, by_x, *far], norm_gain, fsdp_size)
        near_lengths = [send(lengths, to_y), send(lengths, to_x), send(lengths, to_xy)]
        normed, *near_lengths = lax.optimization_barrier((normed, *near_lengths))
        group_lengths = jnp.stack([lengths, *near_lengths])[:, 0]
        acc = None
        for (plane, own, _), other in zip(qkv_blocks, others):
            for core, weights in ((c, own), (1 - c, other)):
                part = jnp.dot(
                    lax.dynamic_index_in_dim(
                        normed, jnp.maximum(plane, 0) * 2 + core, 0, False
                    ),
                    weights,
                    preferred_element_type=jnp.float32,
                )
                acc = part if acc is None else acc + part

        attn = attend(
            acc,
            group_slices(qkv_bias, g, 0),
            rotary_tables(length_rows),
            group_lengths,
            query_heads,
            length_rows,
        )

        cut = lax.dynamic_slice_in_dim(
            out_weight.T, jnp.where(near, g, g ^ 1) * query_cols, query_cols, 1
        )
        out_blocks = spread(with_hop(cut), attn)
        groups = [[], [], []]
        for index, (_, own, step) in enumerate(out_blocks):
            other = send(own, to_core)
            weights = jnp.where(
                c == 0,
                jnp.concatenate([own, other], axis=0),
                jnp.concatenate([other, own], axis=0),
            )
            part = lax.dot_general(
                attn, weights, (((1,), (1,)), ((), ())), preferred_element_type=jnp.float32
            ).astype(jnp.bfloat16)
            at = 0 if 2 * step < planes else 1
            groups[2 if index == len(out_blocks) - 1 else at].append(part)
        groups = [group for group in groups if group]
        pieces = []
        for j, move in enumerate((None, to_y, to_x, to_xy)):
            for group in groups:
                rows = slice(j * length_rows, (j + 1) * length_rows)
                piece = jnp.stack([part[rows] for part in group])
                pieces.append(piece if move is None else send(piece, move))
        counted = []
        for group in (0, 1, 2):
            for index, (plane, _, step) in enumerate(out_blocks):
                at = 0 if 2 * step < planes else 1
                if group == (2 if index == len(out_blocks) - 1 else at):
                    counted.append(plane)
        slots = [
            sum(b * (plane == p).astype(jnp.int32) for b, plane in enumerate(counted))
            for p in range(planes)
        ]
        place = jnp.stack([length, *slots]).astype(jnp.int32)
        hidden, scored = finish(place, sequence, final_gain, value_head, pieces, len(groups))
        score = scored[0, 0]

        total_seqs = fsdp_size * dp_size
        index_all = jnp.arange(total_seqs, dtype=jnp.int32)
        mine = f * dp_size + d
        lane = lax.broadcasted_iota(jnp.int32, (total_seqs, 1, 128), 2)
        both = jnp.where(lane == 0, score, pair_weight[0])
        gathered = lax.all_to_all(both, AXES, 0, 0, tiled=True)
        everyone = gathered[:, 0, 0]
        weights_all = gathered[:, 0, 1]
        matches = partner[:, None] == index_all[None, :]
        others_all = jnp.sum(jnp.where(matches, everyone[None, :], jnp.float32(0.0)), axis=1)
        margins_all = jnp.where(index_all < partner, everyone - others_all, others_all - everyone)
        margin = jnp.sum(jnp.where(index_all == mine, margins_all, 0.0))
        loss = jnp.sum(weights_all * jax.nn.softplus(-margins_all)) / total_seqs
        return (hidden[None], margin.reshape(1), loss)


    return jax.shard_map(
        whole,
        mesh=mesh,
        in_specs=(
            P(("fsdp", "dp"), None, None),
            P(("fsdp", "dp")),
            P(),
            P(("fsdp", "dp")),
            P(),
            P("fsdp", None),
            P(),
            P(None, "fsdp"),
            P(),
            P(),
        ),
        out_specs=(P(("fsdp", "dp"), None, None), P(("fsdp", "dp")), P()),
        check_vma=False,
    )
```

```python
import jax
import jax.numpy as jnp
from jax import lax
from jax.experimental import pallas as pl
from jax.experimental.pallas import tpu as pltpu
from jax.sharding import PartitionSpec as P


QUERY_HEADS = 28
KEY_VALUE_HEADS = 4
HEAD_SIZE = 128
QUERY_FEATURES = 3584
KEY_FEATURES = 512
AXES = ("fsdp", "dp")


def rms_scale(value_rows, gain):
    return (
        value_rows
        * lax.rsqrt(jnp.mean(value_rows * value_rows, axis=-1, keepdims=True) + 1e-06)
        * gain
    )


def rotary_tables(length_rows):
    half = HEAD_SIZE // 2
    positions = jnp.arange(length_rows, dtype=jnp.float32)
    freqs = jnp.exp(
        -(2.0 * jnp.arange(half, dtype=jnp.float32) / HEAD_SIZE) * jnp.log(jnp.float32(1000000.0))
    )
    angles = positions[:, None] * freqs[None, :]
    cosine = jnp.cos(angles)
    sine = jnp.sin(angles)
    return (
        jnp.concatenate([cosine, cosine], axis=-1),
        jnp.concatenate([-sine, sine], axis=-1),
    )


def attention_kernel(
    query_heads, lengths_ref, acc_ref, bias_ref, cos_ref, sin_ref, out_ref
):
    length = lengths_ref[pl.program_id(0)]
    rows = acc_ref.shape[0]
    cosine = cos_ref[...]
    sine = sin_ref[...]

    def head(index):
        cols = pl.ds(index * HEAD_SIZE, HEAD_SIZE)
        return acc_ref[:, cols] + bias_ref[:, cols]

    def rotate(values):
        return (
            values * cosine + pltpu.roll(values, HEAD_SIZE // 2, 1) * sine
        ).astype(jnp.bfloat16)

    key_rows = rotate(head(query_heads))
    value_rows = head(query_heads + 1).astype(jnp.bfloat16)
    row = lax.broadcasted_iota(jnp.int32, (rows, rows), 0)
    col = lax.broadcasted_iota(jnp.int32, (rows, rows), 1)
    allowed = (col <= row) & (col < length)
    scale = 1.0 / jnp.sqrt(jnp.float32(HEAD_SIZE))
    scores = []
    for index in range(query_heads):
        raw = lax.dot_general(
            rotate(head(index)),
            key_rows,
            (((1,), (1,)), ((), ())),
            preferred_element_type=jnp.float32,
        )
        scores.append(jnp.where(allowed, raw * scale, jnp.float32(-1e30)))
    probs = []
    for score in scores:
        expd = jnp.exp(score - jnp.max(score, axis=-1, keepdims=True))
        inverse = 1.0 / jnp.sum(expd, axis=-1, keepdims=True)
        probs.append((expd * inverse).astype(jnp.bfloat16))
    for index, prob in enumerate(probs):
        mixed = jnp.dot(prob, value_rows, preferred_element_type=jnp.float32)
        out_ref[:, pl.ds(index * HEAD_SIZE, HEAD_SIZE)] = mixed.astype(jnp.bfloat16)


def attend(acc, bias_cols, tables, group_lengths, query_heads, length_rows):
    total_rows, width = acc.shape
    seq_count = total_rows // length_rows
    query_cols = query_heads * HEAD_SIZE

    def kernel(*refs):
        attention_kernel(query_heads, *refs)

    return pl.pallas_call(
        kernel,
        name="attention",
        out_shape=jax.ShapeDtypeStruct((total_rows, query_cols), jnp.bfloat16),
        grid_spec=pltpu.PrefetchScalarGridSpec(
            num_scalar_prefetch=1,
            grid=(seq_count,),
            in_specs=[
                pl.BlockSpec((length_rows, width), lambda i, lengths: (i, 0)),
                pl.BlockSpec((1, width), lambda i, lengths: (0, 0)),
                pl.BlockSpec((length_rows, HEAD_SIZE), lambda i, lengths: (0, 0)),
                pl.BlockSpec((length_rows, HEAD_SIZE), lambda i, lengths: (0, 0)),
            ],
            out_specs=pl.BlockSpec((length_rows, query_cols), lambda i, lengths: (i, 0)),
        ),
        cost_estimate=pl.CostEstimate(
            flops=32 * seq_count * query_heads * length_rows * length_rows * HEAD_SIZE,
            bytes_accessed=acc.size * 4 + total_rows * query_cols * 2,
            transcendentals=seq_count * query_heads * length_rows * length_rows,
        ),
    )(group_lengths, acc, bias_cols.reshape(1, width), *tables)


def norm_kernel(own_ref, by_y_ref, by_x_ref, far_a_ref, far_b_ref, gain_ref, out_ref):
    shards, _, shard_rows = out_ref.shape
    step = far_a_ref.shape[0]
    base = 0
    for source in (own_ref, by_y_ref, by_x_ref, far_a_ref, far_b_ref):

        def body(i, carry, source=source, base=base):
            start = pl.multiple_of(i * step, step)
            values = source[pl.ds(start, step), :].astype(jnp.float32)
            normed = rms_scale(values, gain_ref[...]).astype(jnp.bfloat16)
            target = pl.ds(pl.multiple_of(base + i * step, step), step)
            for s in range(shards):
                out_ref[s, target, :] = normed[:, s * shard_rows : (s + 1) * shard_rows]
            return carry

        lax.fori_loop(0, source.shape[0] // step, body, 0)
        base += source.shape[0]


def normalise(parts, gain, shards):
    rows = sum(part.shape[0] for part in parts)
    width = gain.shape[0]
    return pl.pallas_call(
        norm_kernel,
        name="normalise",
        out_shape=jax.ShapeDtypeStruct((shards, rows, width // shards), jnp.bfloat16),
        cost_estimate=pl.CostEstimate(
            flops=8 * rows * width, bytes_accessed=4 * rows * width, transcendentals=rows
        ),
    )(*parts, gain.reshape(1, width))


def finish_kernel(groups, place_ref, tokens_ref, gain_ref, head_ref, *refs):
    pieces, hidden_ref, score_ref = refs[:-2], refs[-2], refs[-1]
    length = place_ref[0]
    rows, width = tokens_ref.shape
    planes = place_ref.shape[0] - 1
    wide = width // planes
    square = jnp.zeros((1, 1), jnp.float32)
    dotted = jnp.zeros((1, 1), jnp.float32)
    picked = lax.broadcasted_iota(jnp.int32, (rows, 1), 0) == length - 1
    gained = gain_ref[...] * head_ref[...]
    for plane in range(planes):
        slot = place_ref[1 + plane]
        cols = slice(plane * wide, (plane + 1) * wide)
        total = tokens_ref[:, cols].astype(jnp.float32)
        for first in range(0, len(pieces), groups):
            value = None
            base = 0
            for ref in pieces[first : first + groups]:
                count = ref.shape[0]
                part = ref[jnp.clip(slot - base, 0, count - 1)]
                value = part if value is None else jnp.where(slot >= base, part, value)
                base += count
            total += value.astype(jnp.float32)
        hidden = total.astype(jnp.bfloat16)
        hidden_ref[:, cols] = hidden
        last = jnp.sum(jnp.where(picked, hidden.astype(jnp.float32), 0.0), axis=0, keepdims=True)
        square += jnp.sum(last * last, axis=1, keepdims=True)
        dotted += jnp.sum(last * gained[:, cols], axis=1, keepdims=True)
    score_ref[...] = jnp.broadcast_to(
        dotted * lax.rsqrt(square / width + 1e-06), score_ref.shape
    )


def finish(place, tokens, gain, head, pieces, groups):
    rows, width = tokens.shape

    def kernel(*refs):
        finish_kernel(groups, *refs)

    return pl.pallas_call(
        kernel,
        name="finish",
        out_shape=(
            jax.ShapeDtypeStruct((rows, width), jnp.bfloat16),
            jax.ShapeDtypeStruct((1, 128), jnp.float32),
        ),
        in_specs=[pl.BlockSpec(memory_space=pltpu.SMEM)]
        + [pl.BlockSpec(memory_space=pltpu.VMEM)] * (3 + len(pieces)),
        cost_estimate=pl.CostEstimate(
            flops=8 * rows * width, bytes_accessed=6 * rows * width, transcendentals=1
        ),
    )(place, tokens, gain.reshape(1, width), head.reshape(1, width), *pieces)


def solution(mesh):
    fsdp_size = mesh.shape["fsdp"]
    dp_size = mesh.shape["dp"]
    planes = fsdp_size // 2
    ranks = dp_size
    query_heads = QUERY_HEADS // ranks
    key_value_heads = KEY_VALUE_HEADS // ranks
    query_cols = query_heads * HEAD_SIZE
    key_cols = key_value_heads * HEAD_SIZE

    def route(move):
        pairs = []
        for f in range(fsdp_size):
            for d in range(dp_size):
                target = move(f // 2, f % 2, d // 2, d % 2)
                if target is not None:
                    z, y, x, c = target
                    pairs.append((f * dp_size + d, (z * 2 + y) * dp_size + x * 2 + c))
        return pairs

    def send(array, move):
        return lax.ppermute(array, AXES, route(move))

    def to_y(z, y, x, c):
        return (z, 1 - y, x, c)

    def to_x(z, y, x, c):
        return (z, y, x ^ 1, c)

    def to_xy(z, y, x, c):
        return (z, 1 - y, x ^ 1, c)

    def to_core(z, y, x, c):
        return (z, y, x, 1 - c)

    def hop_y(z, y, x, c):
        return (z, 1 - y, x, 1 - c) if c != y else None

    def along(shift, holds):
        def move(z, y, x, c):
            return (z + shift, y, x, c) if holds(z) and 0 <= z + shift < planes else None

        return move

    def outward(step):
        def move(z, y, x, c):
            if z >= step - 1:
                return (z + 1, y, x, c) if z + 1 < planes else None
            if z + step <= planes:
                return (z - 1, y, x, c) if z >= 1 else None
            return None

        return move

    def whole(
        tokens,
        lengths,
        partner,
        pair_weight,
        norm_gain,
        qkv_weight,
        qkv_bias,
        out_weight,
        final_gain,
        value_head,
    ):
        f = lax.axis_index("fsdp")
        d = lax.axis_index("dp")
        z, y, x, c = f // 2, f % 2, d // 2, d % 2
        g = x * 2 + y
        sequence = tokens[0]
        length = lengths[0]
        length_rows, _ = sequence.shape

        def group_slices(array, group, dim):
            return jnp.concatenate(
                [
                    lax.dynamic_slice_in_dim(array, group * query_cols, query_cols, dim),
                    lax.dynamic_slice_in_dim(
                        array, QUERY_FEATURES + group * key_cols, key_cols, dim
                    ),
                    lax.dynamic_slice_in_dim(
                        array, QUERY_FEATURES + KEY_FEATURES + group * key_cols, key_cols, dim
                    ),
                ],
                axis=dim,
            )

        def spread(own, gate=None):
            found = [(z, own, 0)]
            up = down = merged = own
            for step in range(1, planes):
                low, high = z >= step, z + step < planes
                below = jnp.where(low, z - step, -1)
                above = jnp.where(high, z + step, -1)
                if 2 * step <= planes:
                    go_up = along(1, lambda p, step=step: p >= step - 1)
                    go_down = along(-1, lambda p, step=step: p + step <= planes)
                    up = send(up, go_up)
                    down = send(down, go_down)
                    if step == 1 and gate is not None:
                        up, down, _ = lax.optimization_barrier((up, down, gate))
                    if 2 * step < planes:
                        found += [(below, up, step), (above, down, step)]
                        continue
                    merged = jnp.where(low, up, down)
                else:
                    merged = send(merged, outward(step))
                found.append((jnp.where(low, below, above), merged, step))
            return found

        near = c == y

        def with_hop(cut):
            return jnp.where(near, cut, send(cut, hop_y))

        block = with_hop(group_slices(qkv_weight, jnp.where(near, g, g ^ 1), 1))
        qkv_blocks = spread(block)
        others = [send(own, to_core) for _, own, _ in qkv_blocks]

        half = length_rows // 2
        by_y = send(sequence, to_y)
        by_x = send(sequence, to_x)
        halves = by_x[:half], by_y[half:]
        far = [send(halves[0], to_y), send(halves[1], to_x)]
        normed = normalise([sequence, by_y, by_x, *far], norm_gain, fsdp_size)
        near_lengths = [send(lengths, to_y), send(lengths, to_x), send(lengths, to_xy)]
        normed, *near_lengths = lax.optimization_barrier((normed, *near_lengths))
        group_lengths = jnp.stack([lengths, *near_lengths])[:, 0]
        acc = None
        for (plane, own, _), other in zip(qkv_blocks, others):
            for core, weights in ((c, own), (1 - c, other)):
                part = jnp.dot(
                    lax.dynamic_index_in_dim(
                        normed, jnp.maximum(plane, 0) * 2 + core, 0, False
                    ),
                    weights,
                    preferred_element_type=jnp.float32,
                )
                acc = part if acc is None else acc + part

        attn = attend(
            acc,
            group_slices(qkv_bias, g, 0),
            rotary_tables(length_rows),
            group_lengths,
            query_heads,
            length_rows,
        )

        cut = lax.dynamic_slice_in_dim(
            out_weight.T, jnp.where(near, g, g ^ 1) * query_cols, query_cols, 1
        )
        out_blocks = spread(with_hop(cut), attn)
        groups = [[], [], []]
        for index, (_, own, step) in enumerate(out_blocks):
            other = send(own, to_core)
            weights = jnp.where(
                c == 0,
                jnp.concatenate([own, other], axis=0),
                jnp.concatenate([other, own], axis=0),
            )
            part = lax.dot_general(
                attn, weights, (((1,), (1,)), ((), ())), preferred_element_type=jnp.float32
            ).astype(jnp.bfloat16)
            at = 0 if 2 * step < planes else 1
            groups[2 if index == len(out_blocks) - 1 else at].append(part)
        groups = [group for group in groups if group]
        pieces = []
        for j, move in enumerate((None, to_y, to_x, to_xy)):
            for group in groups:
                rows = slice(j * length_rows, (j + 1) * length_rows)
                piece = jnp.stack([part[rows] for part in group])
                pieces.append(piece if move is None else send(piece, move))
        counted = []
        for group in (0, 1, 2):
            for index, (plane, _, step) in enumerate(out_blocks):
                at = 0 if 2 * step < planes else 1
                if group == (2 if index == len(out_blocks) - 1 else at):
                    counted.append(plane)
        slots = [
            sum(b * (plane == p).astype(jnp.int32) for b, plane in enumerate(counted))
            for p in range(planes)
        ]
        place = jnp.stack([length, *slots]).astype(jnp.int32)
        hidden, scored = finish(place, sequence, final_gain, value_head, pieces, len(groups))
        score = scored[0, 0]

        total_seqs = fsdp_size * dp_size
        index_all = jnp.arange(total_seqs, dtype=jnp.int32)
        mine = f * dp_size + d
        lane = lax.broadcasted_iota(jnp.int32, (total_seqs, 1, 128), 2)
        both = jnp.where(lane == 0, score, pair_weight[0])
        gathered = lax.all_to_all(both, AXES, 0, 0, tiled=True)
        everyone = gathered[:, 0, 0]
        weights_all = gathered[:, 0, 1]
        matches = partner[:, None] == index_all[None, :]
        others_all = jnp.sum(jnp.where(matches, everyone[None, :], jnp.float32(0.0)), axis=1)
        margins_all = jnp.where(index_all < partner, everyone - others_all, others_all - everyone)
        margin = jnp.sum(jnp.where(index_all == mine, margins_all, 0.0))
        loss = jnp.sum(weights_all * jax.nn.softplus(-margins_all)) / total_seqs
        return (hidden[None], margin.reshape(1), loss)


    return jax.shard_map(
        whole,
        mesh=mesh,
        in_specs=(
            P(("fsdp", "dp"), None, None),
            P(("fsdp", "dp")),
            P(),
            P(("fsdp", "dp")),
            P(),
            P("fsdp", None),
            P(),
            P(None, "fsdp"),
            P(),
            P(),
        ),
        out_specs=(P(("fsdp", "dp"), None, None), P(("fsdp", "dp")), P()),
        check_vma=False,
    )
```

```python
import jax
import jax.numpy as jnp
from jax import lax
from jax.experimental import pallas as pl
from jax.experimental.pallas import tpu as pltpu
from jax.sharding import PartitionSpec as P


QUERY_HEADS = 28
KEY_VALUE_HEADS = 4
HEAD_SIZE = 128
QUERY_FEATURES = 3584
KEY_FEATURES = 512
AXES = ("fsdp", "dp")


def rms_scale(value_rows, gain):
    return (
        value_rows
        * lax.rsqrt(jnp.mean(value_rows * value_rows, axis=-1, keepdims=True) + 1e-06)
        * gain
    )


def rotary_tables(length_rows):
    half = HEAD_SIZE // 2
    positions = jnp.arange(length_rows, dtype=jnp.float32)
    freqs = jnp.exp(
        -(2.0 * jnp.arange(half, dtype=jnp.float32) / HEAD_SIZE) * jnp.log(jnp.float32(1000000.0))
    )
    angles = positions[:, None] * freqs[None, :]
    cosine = jnp.cos(angles)
    sine = jnp.sin(angles)
    return (
        jnp.concatenate([cosine, cosine], axis=-1),
        jnp.concatenate([-sine, sine], axis=-1),
    )


def attention_kernel(
    query_heads, lengths_ref, acc_ref, bias_ref, cos_ref, sin_ref, out_ref
):
    length = lengths_ref[pl.program_id(0)]
    rows = acc_ref.shape[0]
    cosine = cos_ref[...]
    sine = sin_ref[...]

    def head(index):
        cols = pl.ds(index * HEAD_SIZE, HEAD_SIZE)
        return acc_ref[:, cols] + bias_ref[:, cols]

    def rotate(values):
        return (
            values * cosine + pltpu.roll(values, HEAD_SIZE // 2, 1) * sine
        ).astype(jnp.bfloat16)

    key_rows = rotate(head(query_heads))
    value_rows = head(query_heads + 1).astype(jnp.bfloat16)
    row = lax.broadcasted_iota(jnp.int32, (rows, rows), 0)
    col = lax.broadcasted_iota(jnp.int32, (rows, rows), 1)
    allowed = (col <= row) & (col < length)
    scale = 1.0 / jnp.sqrt(jnp.float32(HEAD_SIZE))
    scores = []
    for index in range(query_heads):
        raw = lax.dot_general(
            rotate(head(index)),
            key_rows,
            (((1,), (1,)), ((), ())),
            preferred_element_type=jnp.float32,
        )
        scores.append(jnp.where(allowed, raw * scale, jnp.float32(-1e30)))
    probs = []
    for score in scores:
        expd = jnp.exp(score - jnp.max(score, axis=-1, keepdims=True))
        inverse = 1.0 / jnp.sum(expd, axis=-1, keepdims=True)
        probs.append((expd * inverse).astype(jnp.bfloat16))
    for index, prob in enumerate(probs):
        mixed = jnp.dot(prob, value_rows, preferred_element_type=jnp.float32)
        out_ref[:, pl.ds(index * HEAD_SIZE, HEAD_SIZE)] = mixed.astype(jnp.bfloat16)


def attend(acc, bias_cols, tables, group_lengths, query_heads, length_rows):
    total_rows, width = acc.shape
    seq_count = total_rows // length_rows
    query_cols = query_heads * HEAD_SIZE

    def kernel(*refs):
        attention_kernel(query_heads, *refs)

    return pl.pallas_call(
        kernel,
        name="attention",
        out_shape=jax.ShapeDtypeStruct((total_rows, query_cols), jnp.bfloat16),
        grid_spec=pltpu.PrefetchScalarGridSpec(
            num_scalar_prefetch=1,
            grid=(seq_count,),
            in_specs=[
                pl.BlockSpec((length_rows, width), lambda i, lengths: (i, 0)),
                pl.BlockSpec((1, width), lambda i, lengths: (0, 0)),
                pl.BlockSpec((length_rows, HEAD_SIZE), lambda i, lengths: (0, 0)),
                pl.BlockSpec((length_rows, HEAD_SIZE), lambda i, lengths: (0, 0)),
            ],
            out_specs=pl.BlockSpec((length_rows, query_cols), lambda i, lengths: (i, 0)),
        ),
        cost_estimate=pl.CostEstimate(
            flops=32 * seq_count * query_heads * length_rows * length_rows * HEAD_SIZE,
            bytes_accessed=acc.size * 4 + total_rows * query_cols * 2,
            transcendentals=seq_count * query_heads * length_rows * length_rows,
        ),
    )(group_lengths, acc, bias_cols.reshape(1, width), *tables)


def norm_kernel(own_ref, by_y_ref, by_x_ref, far_a_ref, far_b_ref, gain_ref, out_ref):
    shards, _, shard_rows = out_ref.shape
    step = far_a_ref.shape[0]
    base = 0
    for source in (own_ref, by_y_ref, by_x_ref, far_a_ref, far_b_ref):

        def body(i, carry, source=source, base=base):
            start = pl.multiple_of(i * step, step)
            values = source[pl.ds(start, step), :].astype(jnp.float32)
            normed = rms_scale(values, gain_ref[...]).astype(jnp.bfloat16)
            target = pl.ds(pl.multiple_of(base + i * step, step), step)
            for s in range(shards):
                out_ref[s, target, :] = normed[:, s * shard_rows : (s + 1) * shard_rows]
            return carry

        lax.fori_loop(0, source.shape[0] // step, body, 0)
        base += source.shape[0]


def normalise(parts, gain, shards):
    rows = sum(part.shape[0] for part in parts)
    width = gain.shape[0]
    return pl.pallas_call(
        norm_kernel,
        name="normalise",
        out_shape=jax.ShapeDtypeStruct((shards, rows, width // shards), jnp.bfloat16),
        cost_estimate=pl.CostEstimate(
            flops=8 * rows * width, bytes_accessed=4 * rows * width, transcendentals=rows
        ),
    )(*parts, gain.reshape(1, width))


def finish_kernel(
    groups, width, place_ref, tokens_ref, gained_ref, *refs
):
    pieces, hidden_ref, score_ref, sums_ref = refs[:-3], refs[-3], refs[-2], refs[-1]
    plane = pl.program_id(0)
    length = place_ref[0]
    slot = place_ref[1 + plane]
    rows = tokens_ref.shape[0]
    total = tokens_ref[...].astype(jnp.float32)
    for first in range(0, len(pieces), len(groups)):
        value = None
        for ref, base in zip(pieces[first : first + len(groups)], groups):
            part = ref[0]
            value = part if value is None else jnp.where(slot >= base, part, value)
        total += value.astype(jnp.float32)
    hidden = total.astype(jnp.bfloat16)
    hidden_ref[...] = hidden
    picked = lax.broadcasted_iota(jnp.int32, (rows, 1), 0) == length - 1
    last = jnp.sum(jnp.where(picked, hidden.astype(jnp.float32), 0.0), axis=0, keepdims=True)
    square = jnp.sum(last * last, axis=1, keepdims=True)
    dotted = jnp.sum(last * gained_ref[...], axis=1, keepdims=True)

    @pl.when(plane == 0)
    def _():
        sums_ref[...] = jnp.zeros_like(sums_ref)

    sums_ref[0] += jnp.broadcast_to(square, sums_ref.shape[1:])
    sums_ref[1] += jnp.broadcast_to(dotted, sums_ref.shape[1:])

    @pl.when(plane == pl.num_programs(0) - 1)
    def _():
        score_ref[...] = sums_ref[1] * lax.rsqrt(sums_ref[0] / width + 1e-06)


def finish(place, tokens, gain, head, pieces, counts):
    rows, width = tokens.shape
    planes = place.shape[0] - 1
    wide = width // planes
    groups = [sum(counts[:index]) for index in range(len(counts))]
    gained = jnp.broadcast_to((gain * head).reshape(1, width), (8, width))

    def kernel(*refs):
        finish_kernel(groups, width, *refs)

    def cols(i, place):
        return (0, i)

    def picked(base, count):
        return lambda i, place: (jnp.clip(place[1 + i] - base, 0, count - 1), 0, 0)

    if wide % 128:
        tokens = tokens.reshape(rows, planes, wide).transpose(1, 0, 2)
        gained = gained.reshape(8, planes, wide).transpose(1, 0, 2)
        plane_spec = pl.BlockSpec((None, rows, wide), lambda i, place: (i, 0, 0))
        row_spec = pl.BlockSpec((None, 8, wide), lambda i, place: (i, 0, 0))
        shape = (planes, rows, wide)
    else:
        plane_spec = pl.BlockSpec((rows, wide), cols)
        row_spec = pl.BlockSpec((8, wide), cols)
        shape = (rows, width)
    hidden, score = pl.pallas_call(
        kernel,
        name="finish",
        out_shape=(
            jax.ShapeDtypeStruct(shape, jnp.bfloat16),
            jax.ShapeDtypeStruct((8, 128), jnp.float32),
        ),
        grid_spec=pltpu.PrefetchScalarGridSpec(
            num_scalar_prefetch=1,
            grid=(planes,),
            in_specs=[plane_spec, row_spec]
            + [
                pl.BlockSpec((1, rows, wide), picked(base, count))
                for _ in range(len(pieces) // len(counts))
                for base, count in zip(groups, counts)
            ],
            out_specs=(plane_spec, pl.BlockSpec((8, 128), lambda i, place: (0, 0))),
            scratch_shapes=[pltpu.VMEM((2, 8, 128), jnp.float32)],
        ),
        cost_estimate=pl.CostEstimate(
            flops=8 * rows * width, bytes_accessed=6 * rows * width, transcendentals=1
        ),
    )(place, tokens, gained, *pieces)
    if wide % 128:
        hidden = hidden.transpose(1, 0, 2).reshape(rows, width)
    return hidden, score


def solution(mesh):
    fsdp_size = mesh.shape["fsdp"]
    dp_size = mesh.shape["dp"]
    planes = fsdp_size // 2
    ranks = dp_size
    query_heads = QUERY_HEADS // ranks
    key_value_heads = KEY_VALUE_HEADS // ranks
    query_cols = query_heads * HEAD_SIZE
    key_cols = key_value_heads * HEAD_SIZE

    def route(move):
        pairs = []
        for f in range(fsdp_size):
            for d in range(dp_size):
                target = move(f // 2, f % 2, d // 2, d % 2)
                if target is not None:
                    z, y, x, c = target
                    pairs.append((f * dp_size + d, (z * 2 + y) * dp_size + x * 2 + c))
        return pairs

    def send(array, move):
        return lax.ppermute(array, AXES, route(move))

    def to_y(z, y, x, c):
        return (z, 1 - y, x, c)

    def to_x(z, y, x, c):
        return (z, y, x ^ 1, c)

    def to_xy(z, y, x, c):
        return (z, 1 - y, x ^ 1, c)

    def to_core(z, y, x, c):
        return (z, y, x, 1 - c)

    def hop_y(z, y, x, c):
        return (z, 1 - y, x, 1 - c) if c != y else None

    def along(shift, holds):
        def move(z, y, x, c):
            return (z + shift, y, x, c) if holds(z) and 0 <= z + shift < planes else None

        return move

    def outward(step):
        def move(z, y, x, c):
            if z >= step - 1:
                return (z + 1, y, x, c) if z + 1 < planes else None
            if z + step <= planes:
                return (z - 1, y, x, c) if z >= 1 else None
            return None

        return move

    def whole(
        tokens,
        lengths,
        partner,
        pair_weight,
        norm_gain,
        qkv_weight,
        qkv_bias,
        out_weight,
        final_gain,
        value_head,
    ):
        f = lax.axis_index("fsdp")
        d = lax.axis_index("dp")
        z, y, x, c = f // 2, f % 2, d // 2, d % 2
        g = x * 2 + y
        sequence = tokens[0]
        length = lengths[0]
        length_rows, _ = sequence.shape

        def group_slices(array, group, dim):
            return jnp.concatenate(
                [
                    lax.dynamic_slice_in_dim(array, group * query_cols, query_cols, dim),
                    lax.dynamic_slice_in_dim(
                        array, QUERY_FEATURES + group * key_cols, key_cols, dim
                    ),
                    lax.dynamic_slice_in_dim(
                        array, QUERY_FEATURES + KEY_FEATURES + group * key_cols, key_cols, dim
                    ),
                ],
                axis=dim,
            )

        def spread(own, gate=None):
            found = [(z, own, 0)]
            up = down = merged = own
            for step in range(1, planes):
                low, high = z >= step, z + step < planes
                below = jnp.where(low, z - step, -1)
                above = jnp.where(high, z + step, -1)
                if 2 * step <= planes:
                    go_up = along(1, lambda p, step=step: p >= step - 1)
                    go_down = along(-1, lambda p, step=step: p + step <= planes)
                    up = send(up, go_up)
                    down = send(down, go_down)
                    if step == 1 and gate is not None:
                        up, down, _ = lax.optimization_barrier((up, down, gate))
                    if 2 * step < planes:
                        found += [(below, up, step), (above, down, step)]
                        continue
                    merged = jnp.where(low, up, down)
                else:
                    merged = send(merged, outward(step))
                found.append((jnp.where(low, below, above), merged, step))
            return found

        near = c == y

        def with_hop(cut):
            return jnp.where(near, cut, send(cut, hop_y))

        block = with_hop(group_slices(qkv_weight, jnp.where(near, g, g ^ 1), 1))
        qkv_blocks = spread(block)
        others = [send(own, to_core) for _, own, _ in qkv_blocks]

        half = length_rows // 2
        by_y = send(sequence, to_y)
        by_x = send(sequence, to_x)
        halves = by_x[:half], by_y[half:]
        far = [send(halves[0], to_y), send(halves[1], to_x)]
        normed = normalise([sequence, by_y, by_x, *far], norm_gain, fsdp_size)
        near_lengths = [send(lengths, to_y), send(lengths, to_x), send(lengths, to_xy)]
        normed, *near_lengths = lax.optimization_barrier((normed, *near_lengths))
        group_lengths = jnp.stack([lengths, *near_lengths])[:, 0]
        acc = None
        for (plane, own, _), other in zip(qkv_blocks, others):
            for core, weights in ((c, own), (1 - c, other)):
                part = jnp.dot(
                    lax.dynamic_index_in_dim(normed, jnp.maximum(plane, 0) * 2 + core, 0, False),
                    weights,
                    preferred_element_type=jnp.float32,
                )
                acc = part if acc is None else acc + part

        attn = attend(
            acc,
            group_slices(qkv_bias, g, 0),
            rotary_tables(length_rows),
            group_lengths,
            query_heads,
            length_rows,
        )

        cut = lax.dynamic_slice_in_dim(
            out_weight.T, jnp.where(near, g, g ^ 1) * query_cols, query_cols, 1
        )
        out_blocks = spread(with_hop(cut), attn)
        groups = [[], [], []]
        for index, (_, own, step) in enumerate(out_blocks):
            other = send(own, to_core)
            weights = jnp.where(
                c == 0,
                jnp.concatenate([own, other], axis=0),
                jnp.concatenate([other, own], axis=0),
            )
            part = lax.dot_general(
                attn, weights, (((1,), (1,)), ((), ())), preferred_element_type=jnp.float32
            ).astype(jnp.bfloat16)
            at = 0 if 2 * step < planes else 1
            groups[2 if index == len(out_blocks) - 1 else at].append(part)
        groups = [group for group in groups if group]
        pieces = []
        for j, move in enumerate((None, to_y, to_x, to_xy)):
            for group in groups:
                rows = slice(j * length_rows, (j + 1) * length_rows)
                piece = jnp.stack([part[rows] for part in group])
                pieces.append(piece if move is None else send(piece, move))
        counted = []
        for group in (0, 1, 2):
            for index, (plane, _, step) in enumerate(out_blocks):
                at = 0 if 2 * step < planes else 1
                if group == (2 if index == len(out_blocks) - 1 else at):
                    counted.append(plane)
        slots = [
            sum(b * (plane == p).astype(jnp.int32) for b, plane in enumerate(counted))
            for p in range(planes)
        ]
        place = jnp.stack([length, *slots]).astype(jnp.int32)
        hidden, scored = finish(
            place, sequence, final_gain, value_head, pieces, [len(group) for group in groups]
        )
        score = scored[0, 0]

        total_seqs = fsdp_size * dp_size
        index_all = jnp.arange(total_seqs, dtype=jnp.int32)
        mine = f * dp_size + d
        lane = lax.broadcasted_iota(jnp.int32, (total_seqs, 1, 128), 2)
        both = jnp.where(lane == 0, score, pair_weight[0])
        gathered = lax.all_to_all(both, AXES, 0, 0, tiled=True)
        everyone = gathered[:, 0, 0]
        weights_all = gathered[:, 0, 1]
        matches = partner[:, None] == index_all[None, :]
        others_all = jnp.sum(jnp.where(matches, everyone[None, :], jnp.float32(0.0)), axis=1)
        margins_all = jnp.where(index_all < partner, everyone - others_all, others_all - everyone)
        margin = jnp.sum(jnp.where(index_all == mine, margins_all, 0.0))
        loss = jnp.sum(weights_all * jax.nn.softplus(-margins_all)) / total_seqs
        return (hidden[None], margin.reshape(1), loss)


    return jax.shard_map(
        whole,
        mesh=mesh,
        in_specs=(
            P(("fsdp", "dp"), None, None),
            P(("fsdp", "dp")),
            P(),
            P(("fsdp", "dp")),
            P(),
            P("fsdp", None),
            P(),
            P(None, "fsdp"),
            P(),
            P(),
        ),
        out_specs=(P(("fsdp", "dp"), None, None), P(("fsdp", "dp")), P()),
        check_vma=False,
    )
```

```python
import jax
import jax.numpy as jnp
from jax import lax
from jax.experimental import pallas as pl
from jax.experimental.pallas import tpu as pltpu
from jax.sharding import PartitionSpec as P


QUERY_HEADS = 28
KEY_VALUE_HEADS = 4
HEAD_SIZE = 128
QUERY_FEATURES = 3584
KEY_FEATURES = 512
AXES = ("fsdp", "dp")


def rms_scale(value_rows, gain):
    return (
        value_rows
        * lax.rsqrt(jnp.mean(value_rows * value_rows, axis=-1, keepdims=True) + 1e-06)
        * gain
    )


def rotary_tables(length_rows):
    half = HEAD_SIZE // 2
    positions = jnp.arange(length_rows, dtype=jnp.float32)
    freqs = jnp.exp(
        -(2.0 * jnp.arange(half, dtype=jnp.float32) / HEAD_SIZE) * jnp.log(jnp.float32(1000000.0))
    )
    angles = positions[:, None] * freqs[None, :]
    cosine = jnp.cos(angles)
    sine = jnp.sin(angles)
    return (
        jnp.concatenate([cosine, cosine], axis=-1),
        jnp.concatenate([-sine, sine], axis=-1),
    )


def attention_kernel(
    query_heads, lengths_ref, acc_ref, bias_ref, cos_ref, sin_ref, out_ref
):
    length = lengths_ref[pl.program_id(0)]
    rows = acc_ref.shape[0]
    cosine = cos_ref[...]
    sine = sin_ref[...]

    def head(index):
        cols = pl.ds(index * HEAD_SIZE, HEAD_SIZE)
        return acc_ref[:, cols] + bias_ref[:, cols]

    def rotate(values):
        return (
            values * cosine + pltpu.roll(values, HEAD_SIZE // 2, 1) * sine
        ).astype(jnp.bfloat16)

    key_rows = rotate(head(query_heads))
    value_rows = head(query_heads + 1).astype(jnp.bfloat16)
    row = lax.broadcasted_iota(jnp.int32, (rows, rows), 0)
    col = lax.broadcasted_iota(jnp.int32, (rows, rows), 1)
    allowed = (col <= row) & (col < length)
    scale = 1.0 / jnp.sqrt(jnp.float32(HEAD_SIZE))
    scores = []
    for index in range(query_heads):
        raw = lax.dot_general(
            rotate(head(index)),
            key_rows,
            (((1,), (1,)), ((), ())),
            preferred_element_type=jnp.float32,
        )
        scores.append(jnp.where(allowed, raw * scale, jnp.float32(-1e30)))
    probs = []
    for score in scores:
        expd = jnp.exp(score - jnp.max(score, axis=-1, keepdims=True))
        inverse = 1.0 / jnp.sum(expd, axis=-1, keepdims=True)
        probs.append((expd * inverse).astype(jnp.bfloat16))
    for index, prob in enumerate(probs):
        mixed = jnp.dot(prob, value_rows, preferred_element_type=jnp.float32)
        out_ref[:, pl.ds(index * HEAD_SIZE, HEAD_SIZE)] = mixed.astype(jnp.bfloat16)


def attend(acc, bias_cols, tables, group_lengths, query_heads, length_rows):
    total_rows, width = acc.shape
    seq_count = total_rows // length_rows
    query_cols = query_heads * HEAD_SIZE

    def kernel(*refs):
        attention_kernel(query_heads, *refs)

    return pl.pallas_call(
        kernel,
        name="attention",
        out_shape=jax.ShapeDtypeStruct((total_rows, query_cols), jnp.bfloat16),
        grid_spec=pltpu.PrefetchScalarGridSpec(
            num_scalar_prefetch=1,
            grid=(seq_count,),
            in_specs=[
                pl.BlockSpec((length_rows, width), lambda i, lengths: (i, 0)),
                pl.BlockSpec((1, width), lambda i, lengths: (0, 0)),
                pl.BlockSpec((length_rows, HEAD_SIZE), lambda i, lengths: (0, 0)),
                pl.BlockSpec((length_rows, HEAD_SIZE), lambda i, lengths: (0, 0)),
            ],
            out_specs=pl.BlockSpec((length_rows, query_cols), lambda i, lengths: (i, 0)),
        ),
        cost_estimate=pl.CostEstimate(
            flops=32 * seq_count * query_heads * length_rows * length_rows * HEAD_SIZE,
            bytes_accessed=acc.size * 4 + total_rows * query_cols * 2,
            transcendentals=seq_count * query_heads * length_rows * length_rows,
        ),
    )(group_lengths, acc, bias_cols.reshape(1, width), *tables)


def norm_kernel(own_ref, by_y_ref, by_x_ref, far_ref, gain_ref, out_ref):
    shards, _, shard_rows = out_ref.shape
    step = own_ref.shape[0] // 2
    base = 0
    for source in (own_ref, by_y_ref, by_x_ref, far_ref):

        def body(i, carry, source=source, base=base):
            start = pl.multiple_of(i * step, step)
            values = source[pl.ds(start, step), :].astype(jnp.float32)
            normed = rms_scale(values, gain_ref[...]).astype(jnp.bfloat16)
            target = pl.ds(pl.multiple_of(base + i * step, step), step)
            for s in range(shards):
                out_ref[s, target, :] = normed[:, s * shard_rows : (s + 1) * shard_rows]
            return carry

        lax.fori_loop(0, source.shape[0] // step, body, 0)
        base += source.shape[0]


def normalise(parts, gain, shards):
    rows = sum(part.shape[0] for part in parts)
    width = gain.shape[0]
    return pl.pallas_call(
        norm_kernel,
        name="normalise",
        out_shape=jax.ShapeDtypeStruct((shards, rows, width // shards), jnp.bfloat16),
        cost_estimate=pl.CostEstimate(
            flops=8 * rows * width, bytes_accessed=4 * rows * width, transcendentals=rows
        ),
    )(*parts, gain.reshape(1, width))


def finish_kernel(groups, place_ref, tokens_ref, gain_ref, head_ref, *refs):
    pieces, hidden_ref, score_ref = refs[:-2], refs[-2], refs[-1]
    length = place_ref[0]
    rows, width = tokens_ref.shape
    planes = place_ref.shape[0] - 1
    wide = width // planes
    square = jnp.zeros((1, 1), jnp.float32)
    dotted = jnp.zeros((1, 1), jnp.float32)
    picked = lax.broadcasted_iota(jnp.int32, (rows, 1), 0) == length - 1
    gained = gain_ref[...] * head_ref[...]
    for plane in range(planes):
        slot = place_ref[1 + plane]
        cols = slice(plane * wide, (plane + 1) * wide)
        total = tokens_ref[:, cols].astype(jnp.float32)
        for first in range(0, len(pieces), groups):
            value = None
            base = 0
            for ref in pieces[first : first + groups]:
                count = ref.shape[0]
                part = ref[jnp.clip(slot - base, 0, count - 1)]
                value = part if value is None else jnp.where(slot >= base, part, value)
                base += count
            total += value.astype(jnp.float32)
        hidden = total.astype(jnp.bfloat16)
        hidden_ref[:, cols] = hidden
        last = jnp.sum(jnp.where(picked, hidden.astype(jnp.float32), 0.0), axis=0, keepdims=True)
        square += jnp.sum(last * last, axis=1, keepdims=True)
        dotted += jnp.sum(last * gained[:, cols], axis=1, keepdims=True)
    score_ref[...] = jnp.broadcast_to(
        dotted * lax.rsqrt(square / width + 1e-06), score_ref.shape
    )


def finish(place, tokens, gain, head, pieces, groups):
    rows, width = tokens.shape

    def kernel(*refs):
        finish_kernel(groups, *refs)

    return pl.pallas_call(
        kernel,
        name="finish",
        out_shape=(
            jax.ShapeDtypeStruct((rows, width), jnp.bfloat16),
            jax.ShapeDtypeStruct((1, 128), jnp.float32),
        ),
        in_specs=[pl.BlockSpec(memory_space=pltpu.SMEM)]
        + [pl.BlockSpec(memory_space=pltpu.VMEM)] * (3 + len(pieces)),
        cost_estimate=pl.CostEstimate(
            flops=8 * rows * width, bytes_accessed=6 * rows * width, transcendentals=1
        ),
    )(place, tokens, gain.reshape(1, width), head.reshape(1, width), *pieces)


def solution(mesh):
    fsdp_size = mesh.shape["fsdp"]
    dp_size = mesh.shape["dp"]
    planes = fsdp_size // 2
    ranks = dp_size
    query_heads = QUERY_HEADS // ranks
    key_value_heads = KEY_VALUE_HEADS // ranks
    query_cols = query_heads * HEAD_SIZE
    key_cols = key_value_heads * HEAD_SIZE

    def route(move):
        pairs = []
        for f in range(fsdp_size):
            for d in range(dp_size):
                target = move(f // 2, f % 2, d // 2, d % 2)
                if target is not None:
                    z, y, x, c = target
                    pairs.append((f * dp_size + d, (z * 2 + y) * dp_size + x * 2 + c))
        return pairs

    def send(array, move):
        return lax.ppermute(array, AXES, route(move))

    def to_y(z, y, x, c):
        return (z, 1 - y, x, c)

    def to_x(z, y, x, c):
        return (z, y, x ^ 1, c)

    def to_xy(z, y, x, c):
        return (z, 1 - y, x ^ 1, c)

    def to_core(z, y, x, c):
        return (z, y, x, 1 - c)

    def hop_y(z, y, x, c):
        return (z, 1 - y, x, 1 - c) if c != y else (z, y, x, c)

    def along(shift, holds):
        def move(z, y, x, c):
            return (z + shift, y, x, c) if holds(z) and 0 <= z + shift < planes else None

        return move

    def outward(step):
        def move(z, y, x, c):
            if z >= step - 1:
                return (z + 1, y, x, c) if z + 1 < planes else None
            if z + step <= planes:
                return (z - 1, y, x, c) if z >= 1 else None
            return None

        return move

    def whole(
        tokens,
        lengths,
        partner,
        pair_weight,
        norm_gain,
        qkv_weight,
        qkv_bias,
        out_weight,
        final_gain,
        value_head,
    ):
        f = lax.axis_index("fsdp")
        d = lax.axis_index("dp")
        z, y, x, c = f // 2, f % 2, d // 2, d % 2
        g = x * 2 + y
        sequence = tokens[0]
        length = lengths[0]
        length_rows, _ = sequence.shape

        def group_slices(array, group, dim):
            return jnp.concatenate(
                [
                    lax.dynamic_slice_in_dim(array, group * query_cols, query_cols, dim),
                    lax.dynamic_slice_in_dim(
                        array, QUERY_FEATURES + group * key_cols, key_cols, dim
                    ),
                    lax.dynamic_slice_in_dim(
                        array, QUERY_FEATURES + KEY_FEATURES + group * key_cols, key_cols, dim
                    ),
                ],
                axis=dim,
            )

        def spread(own, gate=None):
            found = [(z, own, 0)]
            up = down = merged = own
            for step in range(1, planes):
                low, high = z >= step, z + step < planes
                below = jnp.where(low, z - step, -1)
                above = jnp.where(high, z + step, -1)
                if 2 * step <= planes:
                    go_up = along(1, lambda p, step=step: p >= step - 1)
                    go_down = along(-1, lambda p, step=step: p + step <= planes)
                    up = send(up, go_up)
                    down = send(down, go_down)
                    if step == 1 and gate is not None:
                        up, down, _ = lax.optimization_barrier((up, down, gate))
                    if 2 * step < planes:
                        found += [(below, up, step), (above, down, step)]
                        continue
                    merged = jnp.where(low, up, down)
                else:
                    merged = send(merged, outward(step))
                found.append((jnp.where(low, below, above), merged, step))
            return found

        near = c == y

        cut = group_slices(qkv_weight, jnp.where(near, g, g ^ 1), 1)
        qkv_blocks = [
            (plane, send(block, hop_y))
            for plane, block, _ in spread(cut)
        ]
        others = [send(own, to_core) for _, own in qkv_blocks]

        by_y = send(sequence, to_y)
        by_x = send(sequence, to_x)
        far = send(by_y, to_x)
        normed = normalise([sequence, by_y, by_x, far], norm_gain, fsdp_size)
        near_lengths = [send(lengths, to_y), send(lengths, to_x), send(lengths, to_xy)]
        normed, *near_lengths = lax.optimization_barrier((normed, *near_lengths))
        group_lengths = jnp.stack([lengths, *near_lengths])[:, 0]
        acc = None
        for (plane, own), other in zip(qkv_blocks, others):
            for core, weights in ((c, own), (1 - c, other)):
                part = jnp.dot(
                    lax.dynamic_index_in_dim(normed, jnp.maximum(plane, 0) * 2 + core, 0, False),
                    weights,
                    preferred_element_type=jnp.float32,
                )
                acc = part if acc is None else acc + part

        attn = attend(
            acc,
            group_slices(qkv_bias, g, 0),
            rotary_tables(length_rows),
            group_lengths,
            query_heads,
            length_rows,
        )

        cut = lax.dynamic_slice_in_dim(
            out_weight.T, jnp.where(near, g, g ^ 1) * query_cols, query_cols, 1
        )
        out_blocks = spread(send(cut, hop_y), attn)
        groups = [[], [], []]
        for index, (_, own, step) in enumerate(out_blocks):
            other = send(own, to_core)
            weights = jnp.where(
                c == 0,
                jnp.concatenate([own, other], axis=0),
                jnp.concatenate([other, own], axis=0),
            )
            part = lax.dot_general(
                attn, weights, (((1,), (1,)), ((), ())), preferred_element_type=jnp.float32
            ).astype(jnp.bfloat16)
            at = 0 if 2 * step < planes else 1
            groups[2 if index == len(out_blocks) - 1 else at].append(part)
        groups = [group for group in groups if group]
        pieces = []
        for j, move in enumerate((None, to_y, to_x, to_xy)):
            for group in groups:
                rows = slice(j * length_rows, (j + 1) * length_rows)
                piece = jnp.stack([part[rows] for part in group])
                pieces.append(piece if move is None else send(piece, move))
        counted = []
        for group in (0, 1, 2):
            for index, (plane, _, step) in enumerate(out_blocks):
                at = 0 if 2 * step < planes else 1
                if group == (2 if index == len(out_blocks) - 1 else at):
                    counted.append(plane)
        slots = [
            sum(b * (plane == p).astype(jnp.int32) for b, plane in enumerate(counted))
            for p in range(planes)
        ]
        place = jnp.stack([length, *slots]).astype(jnp.int32)
        hidden, scored = finish(place, sequence, final_gain, value_head, pieces, len(groups))
        score = scored[0, 0]

        total_seqs = fsdp_size * dp_size
        index_all = jnp.arange(total_seqs, dtype=jnp.int32)
        mine = f * dp_size + d
        lane = lax.broadcasted_iota(jnp.int32, (total_seqs, 1, 128), 2)
        both = jnp.where(lane == 0, score, pair_weight[0])
        gathered = lax.all_to_all(both, AXES, 0, 0, tiled=True)
        everyone = gathered[:, 0, 0]
        weights_all = gathered[:, 0, 1]
        matches = partner[:, None] == index_all[None, :]
        others_all = jnp.sum(jnp.where(matches, everyone[None, :], jnp.float32(0.0)), axis=1)
        margins_all = jnp.where(index_all < partner, everyone - others_all, others_all - everyone)
        margin = jnp.sum(jnp.where(index_all == mine, margins_all, 0.0))
        loss = jnp.sum(weights_all * jax.nn.softplus(-margins_all)) / total_seqs
        return (hidden[None], margin.reshape(1), loss)


    return jax.shard_map(
        whole,
        mesh=mesh,
        in_specs=(
            P(("fsdp", "dp"), None, None),
            P(("fsdp", "dp")),
            P(),
            P(("fsdp", "dp")),
            P(),
            P("fsdp", None),
            P(),
            P(None, "fsdp"),
            P(),
            P(),
        ),
        out_specs=(P(("fsdp", "dp"), None, None), P(("fsdp", "dp")), P()),
        check_vma=False,
    )
```

```python
import jax
import jax.numpy as jnp
from jax import lax
from jax.experimental import pallas as pl
from jax.experimental.pallas import tpu as pltpu
from jax.sharding import PartitionSpec as P


QUERY_HEADS = 28
KEY_VALUE_HEADS = 4
HEAD_SIZE = 128
QUERY_FEATURES = 3584
KEY_FEATURES = 512
AXES = ("fsdp", "dp")


def rms_scale(value_rows, gain):
    return (
        value_rows
        * lax.rsqrt(jnp.mean(value_rows * value_rows, axis=-1, keepdims=True) + 1e-06)
        * gain
    )


def rotary_tables(length_rows):
    half = HEAD_SIZE // 2
    positions = jnp.arange(length_rows, dtype=jnp.float32)
    freqs = jnp.exp(
        -(2.0 * jnp.arange(half, dtype=jnp.float32) / HEAD_SIZE) * jnp.log(jnp.float32(1000000.0))
    )
    angles = positions[:, None] * freqs[None, :]
    cosine = jnp.cos(angles)
    sine = jnp.sin(angles)
    return (
        jnp.concatenate([cosine, cosine], axis=-1),
        jnp.concatenate([-sine, sine], axis=-1),
    )


def attention_kernel(
    query_heads, lengths_ref, acc_ref, bias_ref, cos_ref, sin_ref, out_ref
):
    length = lengths_ref[pl.program_id(0)]
    rows = acc_ref.shape[0]
    cosine = cos_ref[...]
    sine = sin_ref[...]

    def head(index):
        cols = pl.ds(index * HEAD_SIZE, HEAD_SIZE)
        return acc_ref[:, cols] + bias_ref[:, cols]

    def rotate(values):
        return (
            values * cosine + pltpu.roll(values, HEAD_SIZE // 2, 1) * sine
        ).astype(jnp.bfloat16)

    key_rows = rotate(head(query_heads))
    value_rows = head(query_heads + 1).astype(jnp.bfloat16)
    row = lax.broadcasted_iota(jnp.int32, (rows, rows), 0)
    col = lax.broadcasted_iota(jnp.int32, (rows, rows), 1)
    allowed = (col <= row) & (col < length)
    scale = 1.0 / jnp.sqrt(jnp.float32(HEAD_SIZE))
    scores = []
    for index in range(query_heads):
        raw = lax.dot_general(
            rotate(head(index)),
            key_rows,
            (((1,), (1,)), ((), ())),
            preferred_element_type=jnp.float32,
        )
        scores.append(jnp.where(allowed, raw * scale, jnp.float32(-1e30)))
    probs = []
    for score in scores:
        expd = jnp.exp(score - jnp.max(score, axis=-1, keepdims=True))
        inverse = 1.0 / jnp.sum(expd, axis=-1, keepdims=True)
        probs.append((expd * inverse).astype(jnp.bfloat16))
    for index, prob in enumerate(probs):
        mixed = jnp.dot(prob, value_rows, preferred_element_type=jnp.float32)
        out_ref[:, pl.ds(index * HEAD_SIZE, HEAD_SIZE)] = mixed.astype(jnp.bfloat16)


def attend(acc, bias_cols, tables, group_lengths, query_heads, length_rows):
    total_rows, width = acc.shape
    seq_count = total_rows // length_rows
    query_cols = query_heads * HEAD_SIZE

    def kernel(*refs):
        attention_kernel(query_heads, *refs)

    return pl.pallas_call(
        kernel,
        name="attention",
        out_shape=jax.ShapeDtypeStruct((total_rows, query_cols), jnp.bfloat16),
        grid_spec=pltpu.PrefetchScalarGridSpec(
            num_scalar_prefetch=1,
            grid=(seq_count,),
            in_specs=[
                pl.BlockSpec((length_rows, width), lambda i, lengths: (i, 0)),
                pl.BlockSpec((1, width), lambda i, lengths: (0, 0)),
                pl.BlockSpec((length_rows, HEAD_SIZE), lambda i, lengths: (0, 0)),
                pl.BlockSpec((length_rows, HEAD_SIZE), lambda i, lengths: (0, 0)),
            ],
            out_specs=pl.BlockSpec((length_rows, query_cols), lambda i, lengths: (i, 0)),
        ),
        cost_estimate=pl.CostEstimate(
            flops=32 * seq_count * query_heads * length_rows * length_rows * HEAD_SIZE,
            bytes_accessed=acc.size * 4 + total_rows * query_cols * 2,
            transcendentals=seq_count * query_heads * length_rows * length_rows,
        ),
    )(group_lengths, acc, bias_cols.reshape(1, width), *tables)


def norm_kernel(own_ref, by_y_ref, by_x_ref, far_ref, gain_ref, out_ref):
    shards, _, shard_rows = out_ref.shape
    step = own_ref.shape[0] // 2
    base = 0
    for source in (own_ref, by_y_ref, by_x_ref, far_ref):

        def body(i, carry, source=source, base=base):
            start = pl.multiple_of(i * step, step)
            values = source[pl.ds(start, step), :].astype(jnp.float32)
            normed = rms_scale(values, gain_ref[...]).astype(jnp.bfloat16)
            target = pl.ds(pl.multiple_of(base + i * step, step), step)
            for s in range(shards):
                out_ref[s, target, :] = normed[:, s * shard_rows : (s + 1) * shard_rows]
            return carry

        lax.fori_loop(0, source.shape[0] // step, body, 0)
        base += source.shape[0]


def normalise(parts, gain, shards):
    rows = sum(part.shape[0] for part in parts)
    width = gain.shape[0]
    return pl.pallas_call(
        norm_kernel,
        name="normalise",
        out_shape=jax.ShapeDtypeStruct((shards, rows, width // shards), jnp.bfloat16),
        cost_estimate=pl.CostEstimate(
            flops=8 * rows * width, bytes_accessed=4 * rows * width, transcendentals=rows
        ),
    )(*parts, gain.reshape(1, width))


def finish_kernel(groups, place_ref, tokens_ref, *refs):
    pieces, hidden_ref = refs[:-1], refs[-1]
    width = tokens_ref.shape[1]
    planes = place_ref.shape[0]
    wide = width // planes
    for plane in range(planes):
        slot = place_ref[plane]
        cols = slice(plane * wide, (plane + 1) * wide)
        total = tokens_ref[:, cols].astype(jnp.float32)
        for first in range(0, len(pieces), groups):
            value = None
            base = 0
            for ref in pieces[first : first + groups]:
                count = ref.shape[0]
                part = ref[jnp.clip(slot - base, 0, count - 1)]
                value = part if value is None else jnp.where(slot >= base, part, value)
                base += count
            total += value.astype(jnp.float32)
        hidden_ref[:, cols] = total.astype(jnp.bfloat16)


def finish(place, tokens, pieces, groups):
    rows, width = tokens.shape

    def kernel(*refs):
        finish_kernel(groups, *refs)

    return pl.pallas_call(
        kernel,
        name="finish",
        out_shape=jax.ShapeDtypeStruct((rows, width), jnp.bfloat16),
        in_specs=[pl.BlockSpec(memory_space=pltpu.SMEM)]
        + [pl.BlockSpec(memory_space=pltpu.VMEM)] * (1 + len(pieces)),
        cost_estimate=pl.CostEstimate(
            flops=8 * rows * width, bytes_accessed=6 * rows * width, transcendentals=0
        ),
    )(place, tokens, *pieces)


def score_kernel(slots_ref, weight_ref, last_ref, gained_ref, *refs):
    rows, out_ref = refs[:-1], refs[-1]
    planes = last_ref.shape[0]
    count = rows[0].shape[0]
    at = lax.broadcasted_iota(jnp.int32, (planes, count), 0)
    slot = jnp.zeros((planes, count), jnp.int32)
    for plane in range(planes):
        slot = jnp.where(at == plane, slots_ref[plane], slot)
    block = lax.broadcasted_iota(jnp.int32, (planes, count), 1)
    chosen = jnp.where(slot == block, 1.0, 0.0).astype(jnp.bfloat16)
    total = last_ref[...].astype(jnp.float32)
    for ref in rows:
        total += jnp.dot(chosen, ref[...], preferred_element_type=jnp.float32)
    total = total.astype(jnp.bfloat16).astype(jnp.float32)

    def summed(values):
        return jnp.sum(jnp.sum(values, axis=1, keepdims=True), axis=0, keepdims=True)

    width = last_ref.shape[0] * last_ref.shape[1]
    score = summed(total * gained_ref[...]) * lax.rsqrt(summed(total * total) / width + 1e-06)
    lane = lax.broadcasted_iota(jnp.int32, out_ref.shape, 1)
    out_ref[...] = jnp.where(lane == 0, score, weight_ref[0])


def score_rows(place, pair_weight, last, gained, ahead, total_seqs):
    return pl.pallas_call(
        score_kernel,
        name="score",
        out_shape=jax.ShapeDtypeStruct((total_seqs, 128), jnp.float32),
        in_specs=[pl.BlockSpec(memory_space=pltpu.SMEM)] * 2
        + [pl.BlockSpec(memory_space=pltpu.VMEM)] * (2 + len(ahead)),
        cost_estimate=pl.CostEstimate(
            flops=8 * gained.size, bytes_accessed=16 * gained.size, transcendentals=1
        ),
    )(place, pair_weight, last, gained, *ahead)


def solution(mesh):
    fsdp_size = mesh.shape["fsdp"]
    dp_size = mesh.shape["dp"]
    planes = fsdp_size // 2
    ranks = dp_size
    query_heads = QUERY_HEADS // ranks
    key_value_heads = KEY_VALUE_HEADS // ranks
    query_cols = query_heads * HEAD_SIZE
    key_cols = key_value_heads * HEAD_SIZE

    def route(move):
        pairs = []
        for f in range(fsdp_size):
            for d in range(dp_size):
                target = move(f // 2, f % 2, d // 2, d % 2)
                if target is not None:
                    z, y, x, c = target
                    pairs.append((f * dp_size + d, (z * 2 + y) * dp_size + x * 2 + c))
        return pairs

    def send(array, move):
        return lax.ppermute(array, AXES, route(move))

    def to_y(z, y, x, c):
        return (z, 1 - y, x, c)

    def to_x(z, y, x, c):
        return (z, y, x ^ 1, c)

    def to_xy(z, y, x, c):
        return (z, 1 - y, x ^ 1, c)

    def to_core(z, y, x, c):
        return (z, y, x, 1 - c)

    def hop_y(z, y, x, c):
        return (z, 1 - y, x, 1 - c) if c != y else None

    def hop_or_stay(z, y, x, c):
        return hop_y(z, y, x, c) or (z, y, x, c)

    def along(shift, holds):
        def move(z, y, x, c):
            return (z + shift, y, x, c) if holds(z) and 0 <= z + shift < planes else None

        return move

    def outward(step):
        def move(z, y, x, c):
            if z >= step - 1:
                return (z + 1, y, x, c) if z + 1 < planes else None
            if z + step <= planes:
                return (z - 1, y, x, c) if z >= 1 else None
            return None

        return move

    def whole(
        tokens,
        lengths,
        partner,
        pair_weight,
        norm_gain,
        qkv_weight,
        qkv_bias,
        out_weight,
        final_gain,
        value_head,
    ):
        f = lax.axis_index("fsdp")
        d = lax.axis_index("dp")
        z, y, x, c = f // 2, f % 2, d // 2, d % 2
        g = x * 2 + y
        sequence = tokens[0]
        length = lengths[0]
        length_rows, _ = sequence.shape

        def group_slices(array, group, dim):
            return jnp.concatenate(
                [
                    lax.dynamic_slice_in_dim(array, group * query_cols, query_cols, dim),
                    lax.dynamic_slice_in_dim(
                        array, QUERY_FEATURES + group * key_cols, key_cols, dim
                    ),
                    lax.dynamic_slice_in_dim(
                        array, QUERY_FEATURES + KEY_FEATURES + group * key_cols, key_cols, dim
                    ),
                ],
                axis=dim,
            )

        def spread(own, gate=None):
            found = [(z, own, 0)]
            up = down = merged = own
            for step in range(1, planes):
                low, high = z >= step, z + step < planes
                below = jnp.where(low, z - step, -1)
                above = jnp.where(high, z + step, -1)
                if 2 * step <= planes:
                    go_up = along(1, lambda p, step=step: p >= step - 1)
                    go_down = along(-1, lambda p, step=step: p + step <= planes)
                    up = send(up, go_up)
                    down = send(down, go_down)
                    if step == 1 and gate is not None:
                        up, down, _ = lax.optimization_barrier((up, down, gate))
                    if 2 * step < planes:
                        found += [(below, up, step), (above, down, step)]
                        continue
                    merged = jnp.where(low, up, down)
                else:
                    merged = send(merged, outward(step))
                found.append((jnp.where(low, below, above), merged, step))
            return found

        near = c == y

        cut = group_slices(qkv_weight, jnp.where(near, g, g ^ 1), 1)
        chain = spread(cut)
        qkv_blocks = [(z, jnp.where(near, cut, send(cut, hop_y)))] + [
            (plane, send(block, hop_or_stay))
            for index, (plane, block, _) in enumerate(chain)
            if index > 0
        ]
        others = [send(own, to_core) for _, own in qkv_blocks]

        by_y = send(sequence, to_y)
        by_x = send(sequence, to_x)
        far = send(by_y, to_x)
        normed = normalise([sequence, by_y, by_x, far], norm_gain, fsdp_size)
        near_lengths = [send(lengths, to_y), send(lengths, to_x), send(lengths, to_xy)]
        normed, *near_lengths = lax.optimization_barrier((normed, *near_lengths))
        group_lengths = jnp.stack([lengths, *near_lengths])[:, 0]
        acc = None
        for (plane, own), other in zip(qkv_blocks, others):
            for core, weights in ((c, own), (1 - c, other)):
                part = jnp.dot(
                    lax.dynamic_index_in_dim(normed, jnp.maximum(plane, 0) * 2 + core, 0, False),
                    weights,
                    preferred_element_type=jnp.float32,
                )
                acc = part if acc is None else acc + part

        attn = attend(
            acc,
            group_slices(qkv_bias, g, 0),
            rotary_tables(length_rows),
            group_lengths,
            query_heads,
            length_rows,
        )

        cut = lax.dynamic_slice_in_dim(
            out_weight.T, jnp.where(near, g, g ^ 1) * query_cols, query_cols, 1
        )
        out_blocks = spread(jnp.where(near, cut, send(cut, hop_y)), attn)
        groups = [[], [], []]
        for index, (_, own, step) in enumerate(out_blocks):
            other = send(own, to_core)
            weights = jnp.where(
                c == 0,
                jnp.concatenate([own, other], axis=0),
                jnp.concatenate([other, own], axis=0),
            )
            part = lax.dot_general(
                attn, weights, (((1,), (1,)), ((), ())), preferred_element_type=jnp.float32
            ).astype(jnp.bfloat16)
            at = 0 if 2 * step < planes else 1
            groups[2 if index == len(out_blocks) - 1 else at].append(part)
        groups = [group for group in groups if group]
        parts = [part for group in groups for part in group]
        ahead = []
        for j, move in enumerate((None, to_y, to_x, to_xy)):
            at = j * length_rows + group_lengths[j] - 1
            chosen = jnp.concatenate(
                [lax.dynamic_slice_in_dim(part, at, 1, 0) for part in parts], axis=0
            )
            ahead.append(chosen if move is None else send(chosen, move))
        pieces = []
        for j, move in enumerate((None, to_y, to_x, to_xy)):
            for group in groups:
                rows = slice(j * length_rows, (j + 1) * length_rows)
                piece = jnp.stack([part[rows] for part in group])
                pieces.append(piece if move is None else send(piece, move))
        counted = []
        for group in (0, 1, 2):
            for index, (plane, _, step) in enumerate(out_blocks):
                at = 0 if 2 * step < planes else 1
                if group == (2 if index == len(out_blocks) - 1 else at):
                    counted.append(plane)
        slots = [
            sum(b * (plane == p).astype(jnp.int32) for b, plane in enumerate(counted))
            for p in range(planes)
        ]
        place = jnp.stack(slots).astype(jnp.int32)
        hidden = finish(place, sequence, pieces, len(groups))
        last = lax.dynamic_slice_in_dim(sequence, length - 1, 1, 0).reshape(planes, -1)
        gained = (final_gain * value_head).reshape(planes, -1)
        total_seqs = fsdp_size * dp_size
        both = score_rows(place, pair_weight, last, gained, ahead, total_seqs)

        index_all = jnp.arange(total_seqs, dtype=jnp.int32)
        mine = f * dp_size + d
        gathered = lax.all_to_all(both, AXES, 0, 0, tiled=True)
        everyone = gathered[:, 0]
        weights_all = gathered[:, 1]
        matches = partner[:, None] == index_all[None, :]
        others_all = jnp.sum(jnp.where(matches, everyone[None, :], jnp.float32(0.0)), axis=1)
        margins_all = jnp.where(index_all < partner, everyone - others_all, others_all - everyone)
        margin = jnp.sum(jnp.where(index_all == mine, margins_all, 0.0))
        loss = jnp.sum(weights_all * jax.nn.softplus(-margins_all)) / total_seqs
        return (hidden[None], margin.reshape(1), loss)


    return jax.shard_map(
        whole,
        mesh=mesh,
        in_specs=(
            P(("fsdp", "dp"), None, None),
            P(("fsdp", "dp")),
            P(),
            P(("fsdp", "dp")),
            P(),
            P("fsdp", None),
            P(),
            P(None, "fsdp"),
            P(),
            P(),
        ),
        out_specs=(P(("fsdp", "dp"), None, None), P(("fsdp", "dp")), P()),
        check_vma=False,
    )
```

```python
import jax
import jax.numpy as jnp
from jax import lax
from jax.experimental import pallas as pl
from jax.experimental.pallas import tpu as pltpu
from jax.sharding import PartitionSpec as P


QUERY_HEADS = 28
KEY_VALUE_HEADS = 4
HEAD_SIZE = 128
QUERY_FEATURES = 3584
KEY_FEATURES = 512
AXES = ("fsdp", "dp")


def rms_scale(value_rows, gain):
    return (
        value_rows
        * lax.rsqrt(jnp.mean(value_rows * value_rows, axis=-1, keepdims=True) + 1e-06)
        * gain
    )


def rotary_tables(length_rows):
    half = HEAD_SIZE // 2
    positions = jnp.arange(length_rows, dtype=jnp.float32)
    freqs = jnp.exp(
        -(2.0 * jnp.arange(half, dtype=jnp.float32) / HEAD_SIZE) * jnp.log(jnp.float32(1000000.0))
    )
    angles = positions[:, None] * freqs[None, :]
    cosine = jnp.cos(angles)
    sine = jnp.sin(angles)
    return (
        jnp.concatenate([cosine, cosine], axis=-1),
        jnp.concatenate([-sine, sine], axis=-1),
    )


def attention_kernel(
    query_heads, lengths_ref, acc_ref, bias_ref, cos_ref, sin_ref, out_ref
):
    length = lengths_ref[pl.program_id(0)]
    rows = acc_ref.shape[0]
    cosine = cos_ref[...]
    sine = sin_ref[...]

    def head(index):
        cols = pl.ds(index * HEAD_SIZE, HEAD_SIZE)
        return acc_ref[:, cols] + bias_ref[:, cols]

    def rotate(values):
        return (
            values * cosine + pltpu.roll(values, HEAD_SIZE // 2, 1) * sine
        ).astype(jnp.bfloat16)

    key_rows = rotate(head(query_heads))
    value_rows = head(query_heads + 1).astype(jnp.bfloat16)
    row = lax.broadcasted_iota(jnp.int32, (rows, rows), 0)
    col = lax.broadcasted_iota(jnp.int32, (rows, rows), 1)
    allowed = (col <= row) & (col < length)
    scale = 1.0 / jnp.sqrt(jnp.float32(HEAD_SIZE))
    scores = []
    for index in range(query_heads):
        raw = lax.dot_general(
            rotate(head(index)),
            key_rows,
            (((1,), (1,)), ((), ())),
            preferred_element_type=jnp.float32,
        )
        scores.append(jnp.where(allowed, raw * scale, jnp.float32(-1e30)))
    probs = []
    for score in scores:
        expd = jnp.exp(score - jnp.max(score, axis=-1, keepdims=True))
        inverse = 1.0 / jnp.sum(expd, axis=-1, keepdims=True)
        probs.append((expd * inverse).astype(jnp.bfloat16))
    for index, prob in enumerate(probs):
        mixed = jnp.dot(prob, value_rows, preferred_element_type=jnp.float32)
        out_ref[:, pl.ds(index * HEAD_SIZE, HEAD_SIZE)] = mixed.astype(jnp.bfloat16)


def attend(acc, bias_cols, tables, group_lengths, query_heads, length_rows):
    total_rows, width = acc.shape
    seq_count = total_rows // length_rows
    query_cols = query_heads * HEAD_SIZE

    def kernel(*refs):
        attention_kernel(query_heads, *refs)

    return pl.pallas_call(
        kernel,
        name="attention",
        out_shape=jax.ShapeDtypeStruct((total_rows, query_cols), jnp.bfloat16),
        grid_spec=pltpu.PrefetchScalarGridSpec(
            num_scalar_prefetch=1,
            grid=(seq_count,),
            in_specs=[
                pl.BlockSpec((length_rows, width), lambda i, lengths: (i, 0)),
                pl.BlockSpec((1, width), lambda i, lengths: (0, 0)),
                pl.BlockSpec((length_rows, HEAD_SIZE), lambda i, lengths: (0, 0)),
                pl.BlockSpec((length_rows, HEAD_SIZE), lambda i, lengths: (0, 0)),
            ],
            out_specs=pl.BlockSpec((length_rows, query_cols), lambda i, lengths: (i, 0)),
        ),
        cost_estimate=pl.CostEstimate(
            flops=32 * seq_count * query_heads * length_rows * length_rows * HEAD_SIZE,
            bytes_accessed=acc.size * 4 + total_rows * query_cols * 2,
            transcendentals=seq_count * query_heads * length_rows * length_rows,
        ),
    )(group_lengths, acc, bias_cols.reshape(1, width), *tables)


def norm_kernel(own_ref, by_y_ref, by_x_ref, far_ref, gain_ref, out_ref):
    shards, _, shard_rows = out_ref.shape
    step = own_ref.shape[0] // 2
    base = 0
    for source in (own_ref, by_y_ref, by_x_ref, far_ref):

        def body(i, carry, source=source, base=base):
            start = pl.multiple_of(i * step, step)
            values = source[pl.ds(start, step), :].astype(jnp.float32)
            normed = rms_scale(values, gain_ref[...]).astype(jnp.bfloat16)
            target = pl.ds(pl.multiple_of(base + i * step, step), step)
            for s in range(shards):
                out_ref[s, target, :] = normed[:, s * shard_rows : (s + 1) * shard_rows]
            return carry

        lax.fori_loop(0, source.shape[0] // step, body, 0)
        base += source.shape[0]


def normalise(parts, gain, shards):
    rows = sum(part.shape[0] for part in parts)
    width = gain.shape[0]
    return pl.pallas_call(
        norm_kernel,
        name="normalise",
        out_shape=jax.ShapeDtypeStruct((shards, rows, width // shards), jnp.bfloat16),
        cost_estimate=pl.CostEstimate(
            flops=8 * rows * width, bytes_accessed=4 * rows * width, transcendentals=rows
        ),
    )(*parts, gain.reshape(1, width))


def finish_kernel(groups, place_ref, tokens_ref, *refs):
    pieces, hidden_ref = refs[:-1], refs[-1]
    width = tokens_ref.shape[1]
    planes = place_ref.shape[0]
    wide = width // planes
    for plane in range(planes):
        slot = place_ref[plane]
        cols = slice(plane * wide, (plane + 1) * wide)
        total = tokens_ref[:, cols].astype(jnp.float32)
        for first in range(0, len(pieces), groups):
            value = None
            base = 0
            for ref in pieces[first : first + groups]:
                count = ref.shape[0]
                part = ref[jnp.clip(slot - base, 0, count - 1)]
                value = part if value is None else jnp.where(slot >= base, part, value)
                base += count
            total += value.astype(jnp.float32)
        hidden_ref[:, cols] = total.astype(jnp.bfloat16)


def finish(place, tokens, pieces, groups):
    rows, width = tokens.shape

    def kernel(*refs):
        finish_kernel(groups, *refs)

    return pl.pallas_call(
        kernel,
        name="finish",
        out_shape=jax.ShapeDtypeStruct((rows, width), jnp.bfloat16),
        in_specs=[pl.BlockSpec(memory_space=pltpu.SMEM)]
        + [pl.BlockSpec(memory_space=pltpu.VMEM)] * (1 + len(pieces)),
        cost_estimate=pl.CostEstimate(
            flops=8 * rows * width, bytes_accessed=6 * rows * width, transcendentals=0
        ),
    )(place, tokens, *pieces)


def score_kernel(slots_ref, weight_ref, last_ref, gained_ref, *refs):
    rows, out_ref = refs[:-1], refs[-1]
    planes = last_ref.shape[0]
    count = rows[0].shape[0]
    at = lax.broadcasted_iota(jnp.int32, (planes, count), 0)
    slot = jnp.zeros((planes, count), jnp.int32)
    for plane in range(planes):
        slot = jnp.where(at == plane, slots_ref[plane], slot)
    block = lax.broadcasted_iota(jnp.int32, (planes, count), 1)
    chosen = jnp.where(slot == block, 1.0, 0.0).astype(jnp.bfloat16)
    total = last_ref[...].astype(jnp.float32)
    for ref in rows:
        total += jnp.dot(chosen, ref[...], preferred_element_type=jnp.float32)
    total = total.astype(jnp.bfloat16).astype(jnp.float32)

    def summed(values):
        return jnp.sum(jnp.sum(values, axis=1, keepdims=True), axis=0, keepdims=True)

    width = last_ref.shape[0] * last_ref.shape[1]
    score = summed(total * gained_ref[...]) * lax.rsqrt(summed(total * total) / width + 1e-06)
    lane = lax.broadcasted_iota(jnp.int32, out_ref.shape, 1)
    out_ref[...] = jnp.where(lane == 0, score, weight_ref[0])


def score_rows(place, pair_weight, last, gained, ahead, total_seqs):
    return pl.pallas_call(
        score_kernel,
        name="score",
        out_shape=jax.ShapeDtypeStruct((total_seqs, 128), jnp.float32),
        in_specs=[pl.BlockSpec(memory_space=pltpu.SMEM)] * 2
        + [pl.BlockSpec(memory_space=pltpu.VMEM)] * (2 + len(ahead)),
        cost_estimate=pl.CostEstimate(
            flops=8 * gained.size, bytes_accessed=16 * gained.size, transcendentals=1
        ),
    )(place, pair_weight, last, gained, *ahead)


def solution(mesh):
    fsdp_size = mesh.shape["fsdp"]
    dp_size = mesh.shape["dp"]
    planes = fsdp_size // 2
    ranks = dp_size
    query_heads = QUERY_HEADS // ranks
    key_value_heads = KEY_VALUE_HEADS // ranks
    query_cols = query_heads * HEAD_SIZE
    key_cols = key_value_heads * HEAD_SIZE

    def route(move):
        pairs = []
        for f in range(fsdp_size):
            for d in range(dp_size):
                target = move(f // 2, f % 2, d // 2, d % 2)
                if target is not None:
                    z, y, x, c = target
                    pairs.append((f * dp_size + d, (z * 2 + y) * dp_size + x * 2 + c))
        return pairs

    def send(array, move):
        return lax.ppermute(array, AXES, route(move))

    def to_y(z, y, x, c):
        return (z, 1 - y, x, c)

    def to_x(z, y, x, c):
        return (z, y, x ^ 1, c)

    def to_xy(z, y, x, c):
        return (z, 1 - y, x ^ 1, c)

    def to_core(z, y, x, c):
        return (z, y, x, 1 - c)

    def hop_y(z, y, x, c):
        return (z, 1 - y, x, 1 - c) if c != y else None

    def along(shift, holds):
        def move(z, y, x, c):
            return (z + shift, y, x, c) if holds(z) and 0 <= z + shift < planes else None

        return move

    def outward(step):
        def move(z, y, x, c):
            if z >= step - 1:
                return (z + 1, y, x, c) if z + 1 < planes else None
            if z + step <= planes:
                return (z - 1, y, x, c) if z >= 1 else None
            return None

        return move

    def whole(
        tokens,
        lengths,
        partner,
        pair_weight,
        norm_gain,
        qkv_weight,
        qkv_bias,
        out_weight,
        final_gain,
        value_head,
    ):
        f = lax.axis_index("fsdp")
        d = lax.axis_index("dp")
        z, y, x, c = f // 2, f % 2, d // 2, d % 2
        g = x * 2 + y
        sequence = tokens[0]
        length = lengths[0]
        length_rows, _ = sequence.shape

        def group_slices(array, group, dim):
            return jnp.concatenate(
                [
                    lax.dynamic_slice_in_dim(array, group * query_cols, query_cols, dim),
                    lax.dynamic_slice_in_dim(
                        array, QUERY_FEATURES + group * key_cols, key_cols, dim
                    ),
                    lax.dynamic_slice_in_dim(
                        array, QUERY_FEATURES + KEY_FEATURES + group * key_cols, key_cols, dim
                    ),
                ],
                axis=dim,
            )

        def spread(own, gate=None):
            found = [(z, own, 0)]
            up = down = merged = own
            for step in range(1, planes):
                low, high = z >= step, z + step < planes
                below = jnp.where(low, z - step, -1)
                above = jnp.where(high, z + step, -1)
                if 2 * step <= planes:
                    go_up = along(1, lambda p, step=step: p >= step - 1)
                    go_down = along(-1, lambda p, step=step: p + step <= planes)
                    up = send(up, go_up)
                    down = send(down, go_down)
                    if step == 1 and gate is not None:
                        up, down, _ = lax.optimization_barrier((up, down, gate))
                    if 2 * step < planes:
                        found += [(below, up, step), (above, down, step)]
                        continue
                    merged = jnp.where(low, up, down)
                else:
                    merged = send(merged, outward(step))
                found.append((jnp.where(low, below, above), merged, step))
            return found

        near = c == y

        cut = group_slices(qkv_weight, jnp.where(near, g, g ^ 1), 1)
        chain = spread(cut)
        qkv_blocks = [
            (plane, jnp.where(near, block, send(block, hop_y)))
            for plane, block, _ in chain
        ]
        others = [send(own, to_core) for _, own in qkv_blocks]

        by_y = send(sequence, to_y)
        by_x = send(sequence, to_x)
        far = send(by_y, to_x)
        normed = normalise([sequence, by_y, by_x, far], norm_gain, fsdp_size)
        near_lengths = [send(lengths, to_y), send(lengths, to_x), send(lengths, to_xy)]
        normed, *near_lengths = lax.optimization_barrier((normed, *near_lengths))
        group_lengths = jnp.stack([lengths, *near_lengths])[:, 0]
        acc = None
        for (plane, own), other in zip(qkv_blocks, others):
            for core, weights in ((c, own), (1 - c, other)):
                part = jnp.dot(
                    lax.dynamic_index_in_dim(normed, jnp.maximum(plane, 0) * 2 + core, 0, False),
                    weights,
                    preferred_element_type=jnp.float32,
                )
                acc = part if acc is None else acc + part

        attn = attend(
            acc,
            group_slices(qkv_bias, g, 0),
            rotary_tables(length_rows),
            group_lengths,
            query_heads,
            length_rows,
        )

        cut = lax.dynamic_slice_in_dim(
            out_weight.T, jnp.where(near, g, g ^ 1) * query_cols, query_cols, 1
        )
        hopped = send(cut, hop_y)
        kept = jnp.where(near, cut, hopped)
        out_blocks = spread(kept, attn)
        groups = [[], [], []]
        for index, (_, own, step) in enumerate(out_blocks):
            other = send(own, to_core)
            weights = jnp.where(
                c == 0,
                jnp.concatenate([own, other], axis=0),
                jnp.concatenate([other, own], axis=0),
            )
            part = lax.dot_general(
                attn, weights, (((1,), (1,)), ((), ())), preferred_element_type=jnp.float32
            ).astype(jnp.bfloat16)
            at = 0 if 2 * step < planes else 1
            groups[2 if index == len(out_blocks) - 1 else at].append(part)
        groups = [group for group in groups if group]
        parts = [part for group in groups for part in group]
        ahead = []
        for j, move in enumerate((None, to_y, to_x, to_xy)):
            at = j * length_rows + group_lengths[j] - 1
            rows = [lax.dynamic_slice_in_dim(part, at, 1, 0) for part in parts]
            chosen = jnp.concatenate(rows, axis=0)
            ahead.append(chosen if move is None else send(chosen, move))
        pieces = []
        for j, move in enumerate((None, to_y, to_x, to_xy)):
            for group in groups:
                rows = slice(j * length_rows, (j + 1) * length_rows)
                piece = jnp.stack([part[rows] for part in group])
                pieces.append(piece if move is None else send(piece, move))
        counted = []
        for group in (0, 1, 2):
            for index, (plane, _, step) in enumerate(out_blocks):
                at = 0 if 2 * step < planes else 1
                if group == (2 if index == len(out_blocks) - 1 else at):
                    counted.append(plane)
        slots = [
            sum(b * (plane == p).astype(jnp.int32) for b, plane in enumerate(counted))
            for p in range(planes)
        ]
        place = jnp.stack(slots).astype(jnp.int32)
        hidden = finish(place, sequence, pieces, len(groups))
        last = lax.dynamic_slice_in_dim(sequence, length - 1, 1, 0).reshape(planes, -1)
        gained = (final_gain * value_head).reshape(planes, -1)
        total_seqs = fsdp_size * dp_size
        both = score_rows(place, pair_weight, last, gained, ahead, total_seqs)

        index_all = jnp.arange(total_seqs, dtype=jnp.int32)
        mine = f * dp_size + d
        gathered = lax.all_to_all(both, AXES, 0, 0, tiled=True)
        everyone = gathered[:, 0]
        weights_all = gathered[:, 1]
        matches = partner[:, None] == index_all[None, :]
        others_all = jnp.sum(jnp.where(matches, everyone[None, :], jnp.float32(0.0)), axis=1)
        margins_all = jnp.where(index_all < partner, everyone - others_all, others_all - everyone)
        margin = jnp.sum(jnp.where(index_all == mine, margins_all, 0.0))
        loss = jnp.sum(weights_all * jax.nn.softplus(-margins_all)) / total_seqs
        return (hidden[None], margin.reshape(1), loss)


    return jax.shard_map(
        whole,
        mesh=mesh,
        in_specs=(
            P(("fsdp", "dp"), None, None),
            P(("fsdp", "dp")),
            P(),
            P(("fsdp", "dp")),
            P(),
            P("fsdp", None),
            P(),
            P(None, "fsdp"),
            P(),
            P(),
        ),
        out_specs=(P(("fsdp", "dp"), None, None), P(("fsdp", "dp")), P()),
        check_vma=False,
    )
```

```python
import jax
import jax.numpy as jnp
from jax import lax
from jax.experimental import pallas as pl
from jax.experimental.pallas import tpu as pltpu
from jax.sharding import PartitionSpec as P


QUERY_HEADS = 28
KEY_VALUE_HEADS = 4
HEAD_SIZE = 128
QUERY_FEATURES = 3584
KEY_FEATURES = 512
AXES = ("fsdp", "dp")


def rms_scale(value_rows, gain):
    return (
        value_rows
        * lax.rsqrt(jnp.mean(value_rows * value_rows, axis=-1, keepdims=True) + 1e-06)
        * gain
    )


def rotary_tables(length_rows):
    half = HEAD_SIZE // 2
    positions = jnp.arange(length_rows, dtype=jnp.float32)
    freqs = jnp.exp(
        -(2.0 * jnp.arange(half, dtype=jnp.float32) / HEAD_SIZE) * jnp.log(jnp.float32(1000000.0))
    )
    angles = positions[:, None] * freqs[None, :]
    cosine = jnp.cos(angles)
    sine = jnp.sin(angles)
    return (
        jnp.concatenate([cosine, cosine], axis=-1),
        jnp.concatenate([-sine, sine], axis=-1),
    )


def attention_kernel(
    query_heads, lengths_refs, acc_ref, bias_ref, cos_ref, sin_ref, out_ref
):
    length = lengths_refs[0][0]
    for index in range(1, len(lengths_refs)):
        length = jnp.where(pl.program_id(0) == index, lengths_refs[index][0], length)
    rows = acc_ref.shape[0]
    cosine = cos_ref[...]
    sine = sin_ref[...]

    def head(index):
        cols = pl.ds(index * HEAD_SIZE, HEAD_SIZE)
        return acc_ref[:, cols] + bias_ref[:, cols]

    def rotate(values):
        return (
            values * cosine + pltpu.roll(values, HEAD_SIZE // 2, 1) * sine
        ).astype(jnp.bfloat16)

    key_rows = rotate(head(query_heads))
    value_rows = head(query_heads + 1).astype(jnp.bfloat16)
    row = lax.broadcasted_iota(jnp.int32, (rows, rows), 0)
    col = lax.broadcasted_iota(jnp.int32, (rows, rows), 1)
    allowed = (col <= row) & (col < length)
    scale = 1.0 / jnp.sqrt(jnp.float32(HEAD_SIZE))
    scores = []
    for index in range(query_heads):
        raw = lax.dot_general(
            rotate(head(index)),
            key_rows,
            (((1,), (1,)), ((), ())),
            preferred_element_type=jnp.float32,
        )
        scores.append(jnp.where(allowed, raw * scale, jnp.float32(-1e30)))
    probs = []
    for score in scores:
        expd = jnp.exp(score - jnp.max(score, axis=-1, keepdims=True))
        inverse = 1.0 / jnp.sum(expd, axis=-1, keepdims=True)
        probs.append((expd * inverse).astype(jnp.bfloat16))
    for index, prob in enumerate(probs):
        mixed = jnp.dot(prob, value_rows, preferred_element_type=jnp.float32)
        out_ref[:, pl.ds(index * HEAD_SIZE, HEAD_SIZE)] = mixed.astype(jnp.bfloat16)


def attend(acc, bias_cols, tables, group_lengths, query_heads, length_rows):
    total_rows, width = acc.shape
    seq_count = total_rows // length_rows
    query_cols = query_heads * HEAD_SIZE

    def kernel(*refs):
        attention_kernel(query_heads, refs[:seq_count], *refs[seq_count:])

    return pl.pallas_call(
        kernel,
        name="attention",
        out_shape=jax.ShapeDtypeStruct((total_rows, query_cols), jnp.bfloat16),
        grid_spec=pltpu.PrefetchScalarGridSpec(
            num_scalar_prefetch=seq_count,
            grid=(seq_count,),
            in_specs=[
                pl.BlockSpec((length_rows, width), lambda i, *lengths: (i, 0)),
                pl.BlockSpec((1, width), lambda i, *lengths: (0, 0)),
                pl.BlockSpec((length_rows, HEAD_SIZE), lambda i, *lengths: (0, 0)),
                pl.BlockSpec((length_rows, HEAD_SIZE), lambda i, *lengths: (0, 0)),
            ],
            out_specs=pl.BlockSpec((length_rows, query_cols), lambda i, *lengths: (i, 0)),
        ),
        cost_estimate=pl.CostEstimate(
            flops=32 * seq_count * query_heads * length_rows * length_rows * HEAD_SIZE,
            bytes_accessed=acc.size * 4 + total_rows * query_cols * 2,
            transcendentals=seq_count * query_heads * length_rows * length_rows,
        ),
    )(*group_lengths, acc, bias_cols.reshape(1, width), *tables)


def norm_kernel(own_ref, by_y_ref, by_x_ref, far_ref, gain_ref, out_ref):
    shards, _, shard_rows = out_ref.shape
    step = own_ref.shape[0] // 2
    base = 0
    for source in (own_ref, by_y_ref, by_x_ref, far_ref):

        def body(i, carry, source=source, base=base):
            start = pl.multiple_of(i * step, step)
            values = source[pl.ds(start, step), :].astype(jnp.float32)
            normed = rms_scale(values, gain_ref[...]).astype(jnp.bfloat16)
            target = pl.ds(pl.multiple_of(base + i * step, step), step)
            for s in range(shards):
                out_ref[s, target, :] = normed[:, s * shard_rows : (s + 1) * shard_rows]
            return carry

        lax.fori_loop(0, source.shape[0] // step, body, 0)
        base += source.shape[0]


def normalise(parts, gain, shards):
    rows = sum(part.shape[0] for part in parts)
    width = gain.shape[0]
    return pl.pallas_call(
        norm_kernel,
        name="normalise",
        out_shape=jax.ShapeDtypeStruct((shards, rows, width // shards), jnp.bfloat16),
        cost_estimate=pl.CostEstimate(
            flops=8 * rows * width, bytes_accessed=4 * rows * width, transcendentals=rows
        ),
    )(*parts, gain.reshape(1, width))


def finish_kernel(groups, place_ref, tokens_ref, *refs):
    pieces, hidden_ref = refs[:-1], refs[-1]
    width = tokens_ref.shape[1]
    planes = place_ref.shape[0]
    wide = width // planes
    for plane in range(planes):
        slot = place_ref[plane]
        cols = slice(plane * wide, (plane + 1) * wide)
        total = tokens_ref[:, cols].astype(jnp.float32)
        for first in range(0, len(pieces), groups):
            value = None
            base = 0
            for ref in pieces[first : first + groups]:
                count = ref.shape[0]
                part = ref[jnp.clip(slot - base, 0, count - 1)]
                value = part if value is None else jnp.where(slot >= base, part, value)
                base += count
            total += value.astype(jnp.float32)
        hidden_ref[:, cols] = total.astype(jnp.bfloat16)


def finish(place, tokens, pieces, groups):
    rows, width = tokens.shape

    def kernel(*refs):
        finish_kernel(groups, *refs)

    return pl.pallas_call(
        kernel,
        name="finish",
        out_shape=jax.ShapeDtypeStruct((rows, width), jnp.bfloat16),
        in_specs=[pl.BlockSpec(memory_space=pltpu.SMEM)]
        + [pl.BlockSpec(memory_space=pltpu.VMEM)] * (1 + len(pieces)),
        cost_estimate=pl.CostEstimate(
            flops=8 * rows * width, bytes_accessed=6 * rows * width, transcendentals=0
        ),
    )(place, tokens, *pieces)


def score_kernel(slots_ref, weight_ref, last_ref, gained_ref, *refs):
    rows, out_ref = refs[:-1], refs[-1]
    planes = last_ref.shape[0]
    count = rows[0].shape[0]
    at = lax.broadcasted_iota(jnp.int32, (planes, count), 0)
    slot = jnp.zeros((planes, count), jnp.int32)
    for plane in range(planes):
        slot = jnp.where(at == plane, slots_ref[plane], slot)
    block = lax.broadcasted_iota(jnp.int32, (planes, count), 1)
    chosen = jnp.where(slot == block, 1.0, 0.0).astype(jnp.bfloat16)
    total = last_ref[...].astype(jnp.float32)
    for ref in rows:
        total += jnp.dot(chosen, ref[...], preferred_element_type=jnp.float32)
    total = total.astype(jnp.bfloat16).astype(jnp.float32)

    def summed(values):
        return jnp.sum(jnp.sum(values, axis=1, keepdims=True), axis=0, keepdims=True)

    width = last_ref.shape[0] * last_ref.shape[1]
    score = summed(total * gained_ref[...]) * lax.rsqrt(summed(total * total) / width + 1e-06)
    lane = lax.broadcasted_iota(jnp.int32, out_ref.shape, 1)
    out_ref[...] = jnp.where(lane == 0, score, weight_ref[0])


def score_rows(place, pair_weight, last, gained, ahead, total_seqs):
    return pl.pallas_call(
        score_kernel,
        name="score",
        out_shape=jax.ShapeDtypeStruct((total_seqs, 128), jnp.float32),
        in_specs=[pl.BlockSpec(memory_space=pltpu.SMEM)] * 2
        + [pl.BlockSpec(memory_space=pltpu.VMEM)] * (2 + len(ahead)),
        cost_estimate=pl.CostEstimate(
            flops=8 * gained.size, bytes_accessed=16 * gained.size, transcendentals=1
        ),
    )(place, pair_weight, last, gained, *ahead)


def solution(mesh):
    fsdp_size = mesh.shape["fsdp"]
    dp_size = mesh.shape["dp"]
    planes = fsdp_size // 2
    ranks = dp_size
    query_heads = QUERY_HEADS // ranks
    key_value_heads = KEY_VALUE_HEADS // ranks
    query_cols = query_heads * HEAD_SIZE
    key_cols = key_value_heads * HEAD_SIZE

    def route(move):
        pairs = []
        for f in range(fsdp_size):
            for d in range(dp_size):
                target = move(f // 2, f % 2, d // 2, d % 2)
                if target is not None:
                    z, y, x, c = target
                    pairs.append((f * dp_size + d, (z * 2 + y) * dp_size + x * 2 + c))
        return pairs

    def send(array, move):
        return lax.ppermute(array, AXES, route(move))

    def to_y(z, y, x, c):
        return (z, 1 - y, x, c)

    def to_x(z, y, x, c):
        return (z, y, x ^ 1, c)

    def to_xy(z, y, x, c):
        return (z, 1 - y, x ^ 1, c)

    def to_core(z, y, x, c):
        return (z, y, x, 1 - c)

    def hop_y(z, y, x, c):
        return (z, 1 - y, x, 1 - c) if c != y else None

    def along(shift, holds):
        def move(z, y, x, c):
            return (z + shift, y, x, c) if holds(z) and 0 <= z + shift < planes else None

        return move

    def outward(step):
        def move(z, y, x, c):
            if z >= step - 1:
                return (z + 1, y, x, c) if z + 1 < planes else None
            if z + step <= planes:
                return (z - 1, y, x, c) if z >= 1 else None
            return None

        return move

    def whole(
        tokens,
        lengths,
        partner,
        pair_weight,
        norm_gain,
        qkv_weight,
        qkv_bias,
        out_weight,
        final_gain,
        value_head,
    ):
        f = lax.axis_index("fsdp")
        d = lax.axis_index("dp")
        z, y, x, c = f // 2, f % 2, d // 2, d % 2
        g = x * 2 + y
        sequence = tokens[0]
        length = lengths[0]
        length_rows, _ = sequence.shape

        def group_slices(array, group, dim):
            return jnp.concatenate(
                [
                    lax.dynamic_slice_in_dim(array, group * query_cols, query_cols, dim),
                    lax.dynamic_slice_in_dim(
                        array, QUERY_FEATURES + group * key_cols, key_cols, dim
                    ),
                    lax.dynamic_slice_in_dim(
                        array, QUERY_FEATURES + KEY_FEATURES + group * key_cols, key_cols, dim
                    ),
                ],
                axis=dim,
            )

        def spread(own, gate=None):
            found = [(z, own, 0)]
            up = down = merged = own
            for step in range(1, planes):
                low, high = z >= step, z + step < planes
                below = jnp.where(low, z - step, -1)
                above = jnp.where(high, z + step, -1)
                if 2 * step <= planes:
                    go_up = along(1, lambda p, step=step: p >= step - 1)
                    go_down = along(-1, lambda p, step=step: p + step <= planes)
                    up = send(up, go_up)
                    down = send(down, go_down)
                    if step == 1 and gate is not None:
                        up, down, _ = lax.optimization_barrier((up, down, gate))
                    if 2 * step < planes:
                        found += [(below, up, step), (above, down, step)]
                        continue
                    merged = jnp.where(low, up, down)
                else:
                    merged = send(merged, outward(step))
                found.append((jnp.where(low, below, above), merged, step))
            return found

        near = c == y

        cut = group_slices(qkv_weight, jnp.where(near, g, g ^ 1), 1)
        chain = spread(cut)
        qkv_blocks = [
            (plane, jnp.where(near, block, send(block, hop_y)))
            for plane, block, _ in chain
        ]
        others = [send(own, to_core) for _, own in qkv_blocks]

        by_y = send(sequence, to_y)
        by_x = send(sequence, to_x)
        far = send(by_y, to_x)
        normed = normalise([sequence, by_y, by_x, far], norm_gain, fsdp_size)
        near_lengths = [send(lengths, to_y), send(lengths, to_x), send(lengths, to_xy)]
        normed, *near_lengths = lax.optimization_barrier((normed, *near_lengths))
        group_lengths = [lengths, *near_lengths]
        acc = None
        for (plane, own), other in zip(qkv_blocks, others):
            for core, weights in ((c, own), (1 - c, other)):
                part = jnp.dot(
                    lax.dynamic_index_in_dim(normed, jnp.maximum(plane, 0) * 2 + core, 0, False),
                    weights,
                    preferred_element_type=jnp.float32,
                )
                acc = part if acc is None else acc + part

        attn = attend(
            acc,
            group_slices(qkv_bias, g, 0),
            rotary_tables(length_rows),
            group_lengths,
            query_heads,
            length_rows,
        )

        cut = lax.dynamic_slice_in_dim(
            out_weight.T, jnp.where(near, g, g ^ 1) * query_cols, query_cols, 1
        )
        hopped = send(cut, hop_y)
        kept = jnp.where(near, cut, hopped)
        out_blocks = spread(kept, attn)
        groups = [[], [], []]
        for index, (_, own, step) in enumerate(out_blocks):
            other = send(own, to_core)
            weights = jnp.where(
                c == 0,
                jnp.concatenate([own, other], axis=0),
                jnp.concatenate([other, own], axis=0),
            )
            part = lax.dot_general(
                attn, weights, (((1,), (1,)), ((), ())), preferred_element_type=jnp.float32
            ).astype(jnp.bfloat16)
            at = 0 if 2 * step < planes else 1
            groups[2 if index == len(out_blocks) - 1 else at].append(part)
        groups = [group for group in groups if group]
        parts = [part for group in groups for part in group]
        ahead = []
        for j, move in enumerate((None, to_y, to_x, to_xy)):
            at = j * length_rows + group_lengths[j][0] - 1
            rows = [lax.dynamic_slice_in_dim(part, at, 1, 0) for part in parts]
            chosen = jnp.concatenate(rows, axis=0)
            ahead.append(chosen if move is None else send(chosen, move))
        pieces = []
        for j, move in enumerate((None, to_y, to_x, to_xy)):
            for group in groups:
                rows = slice(j * length_rows, (j + 1) * length_rows)
                piece = jnp.stack([part[rows] for part in group])
                pieces.append(piece if move is None else send(piece, move))
        counted = []
        for group in (0, 1, 2):
            for index, (plane, _, step) in enumerate(out_blocks):
                at = 0 if 2 * step < planes else 1
                if group == (2 if index == len(out_blocks) - 1 else at):
                    counted.append(plane)
        slots = [
            sum(b * (plane == p).astype(jnp.int32) for b, plane in enumerate(counted))
            for p in range(planes)
        ]
        place = jnp.stack(slots).astype(jnp.int32)
        hidden = finish(place, sequence, pieces, len(groups))
        last = lax.dynamic_slice_in_dim(sequence, length - 1, 1, 0).reshape(planes, -1)
        gained = (final_gain * value_head).reshape(planes, -1)
        total_seqs = fsdp_size * dp_size
        both = score_rows(place, pair_weight, last, gained, ahead, total_seqs)

        index_all = jnp.arange(total_seqs, dtype=jnp.int32)
        mine = f * dp_size + d
        gathered = lax.all_to_all(both, AXES, 0, 0, tiled=True)
        everyone = gathered[:, 0]
        weights_all = gathered[:, 1]
        matches = partner[:, None] == index_all[None, :]
        others_all = jnp.sum(jnp.where(matches, everyone[None, :], jnp.float32(0.0)), axis=1)
        margins_all = jnp.where(index_all < partner, everyone - others_all, others_all - everyone)
        margin = jnp.sum(jnp.where(index_all == mine, margins_all, 0.0))
        loss = jnp.sum(weights_all * jax.nn.softplus(-margins_all)) / total_seqs
        return (hidden[None], margin.reshape(1), loss)


    return jax.shard_map(
        whole,
        mesh=mesh,
        in_specs=(
            P(("fsdp", "dp"), None, None),
            P(("fsdp", "dp")),
            P(),
            P(("fsdp", "dp")),
            P(),
            P("fsdp", None),
            P(),
            P(None, "fsdp"),
            P(),
            P(),
        ),
        out_specs=(P(("fsdp", "dp"), None, None), P(("fsdp", "dp")), P()),
        check_vma=False,
    )
```

```python
import jax
import jax.numpy as jnp
from jax import lax
from jax.experimental import pallas as pl
from jax.experimental.pallas import tpu as pltpu
from jax.sharding import PartitionSpec as P


QUERY_HEADS = 28
KEY_VALUE_HEADS = 4
HEAD_SIZE = 128
QUERY_FEATURES = 3584
KEY_FEATURES = 512
AXES = ("fsdp", "dp")


def rms_scale(value_rows, gain):
    return (
        value_rows
        * lax.rsqrt(jnp.mean(value_rows * value_rows, axis=-1, keepdims=True) + 1e-06)
        * gain
    )


def rotary_tables(length_rows):
    half = HEAD_SIZE // 2
    positions = jnp.arange(length_rows, dtype=jnp.float32)
    freqs = jnp.exp(
        -(2.0 * jnp.arange(half, dtype=jnp.float32) / HEAD_SIZE) * jnp.log(jnp.float32(1000000.0))
    )
    angles = positions[:, None] * freqs[None, :]
    cosine = jnp.cos(angles)
    sine = jnp.sin(angles)
    return (
        jnp.concatenate([cosine, cosine], axis=-1),
        jnp.concatenate([-sine, sine], axis=-1),
    )


def attention_kernel(
    query_heads, lengths_refs, acc_ref, bias_ref, cos_ref, sin_ref, out_ref
):
    length = lengths_refs[0][0]
    for index in range(1, len(lengths_refs)):
        length = jnp.where(pl.program_id(0) == index, lengths_refs[index][0], length)
    rows = acc_ref.shape[0]
    cosine = cos_ref[...]
    sine = sin_ref[...]

    def head(index):
        cols = pl.ds(index * HEAD_SIZE, HEAD_SIZE)
        return acc_ref[:, cols] + bias_ref[:, cols]

    def rotate(values):
        return (
            values * cosine + pltpu.roll(values, HEAD_SIZE // 2, 1) * sine
        ).astype(jnp.bfloat16)

    key_rows = rotate(head(query_heads))
    value_rows = head(query_heads + 1).astype(jnp.bfloat16)
    row = lax.broadcasted_iota(jnp.int32, (rows, rows), 0)
    col = lax.broadcasted_iota(jnp.int32, (rows, rows), 1)
    allowed = (col <= row) & (col < length)
    scale = 1.0 / jnp.sqrt(jnp.float32(HEAD_SIZE))
    scores = []
    for index in range(query_heads):
        raw = lax.dot_general(
            rotate(head(index)),
            key_rows,
            (((1,), (1,)), ((), ())),
            preferred_element_type=jnp.float32,
        )
        scores.append(jnp.where(allowed, raw * scale, jnp.float32(-1e30)))
    probs = []
    for score in scores:
        expd = jnp.exp(score - jnp.max(score, axis=-1, keepdims=True))
        inverse = 1.0 / jnp.sum(expd, axis=-1, keepdims=True)
        probs.append((expd * inverse).astype(jnp.bfloat16))
    for index, prob in enumerate(probs):
        mixed = jnp.dot(prob, value_rows, preferred_element_type=jnp.float32)
        out_ref[:, pl.ds(index * HEAD_SIZE, HEAD_SIZE)] = mixed.astype(jnp.bfloat16)


def attend(acc, bias_cols, tables, group_lengths, query_heads, length_rows):
    total_rows, width = acc.shape
    seq_count = total_rows // length_rows
    query_cols = query_heads * HEAD_SIZE

    def kernel(*refs):
        attention_kernel(query_heads, refs[:seq_count], *refs[seq_count:])

    return pl.pallas_call(
        kernel,
        name="attention",
        out_shape=jax.ShapeDtypeStruct((total_rows, query_cols), jnp.bfloat16),
        grid_spec=pltpu.PrefetchScalarGridSpec(
            num_scalar_prefetch=seq_count,
            grid=(seq_count,),
            in_specs=[
                pl.BlockSpec((length_rows, width), lambda i, *lengths: (i, 0)),
                pl.BlockSpec((1, width), lambda i, *lengths: (0, 0)),
                pl.BlockSpec((length_rows, HEAD_SIZE), lambda i, *lengths: (0, 0)),
                pl.BlockSpec((length_rows, HEAD_SIZE), lambda i, *lengths: (0, 0)),
            ],
            out_specs=pl.BlockSpec((length_rows, query_cols), lambda i, *lengths: (i, 0)),
        ),
        cost_estimate=pl.CostEstimate(
            flops=32 * seq_count * query_heads * length_rows * length_rows * HEAD_SIZE,
            bytes_accessed=acc.size * 4 + total_rows * query_cols * 2,
            transcendentals=seq_count * query_heads * length_rows * length_rows,
        ),
    )(*group_lengths, acc, bias_cols.reshape(1, width), *tables)


def norm_kernel(own_ref, by_y_ref, by_x_ref, far_ref, gain_ref, out_ref):
    shards, _, shard_rows = out_ref.shape
    step = own_ref.shape[0] // 2
    base = 0
    for source in (own_ref, by_y_ref, by_x_ref, far_ref):

        def body(i, carry, source=source, base=base):
            start = pl.multiple_of(i * step, step)
            values = source[pl.ds(start, step), :].astype(jnp.float32)
            normed = rms_scale(values, gain_ref[...]).astype(jnp.bfloat16)
            target = pl.ds(pl.multiple_of(base + i * step, step), step)
            for s in range(shards):
                out_ref[s, target, :] = normed[:, s * shard_rows : (s + 1) * shard_rows]
            return carry

        lax.fori_loop(0, source.shape[0] // step, body, 0)
        base += source.shape[0]


def normalise(parts, gain, shards):
    rows = sum(part.shape[0] for part in parts)
    width = gain.shape[0]
    return pl.pallas_call(
        norm_kernel,
        name="normalise",
        out_shape=jax.ShapeDtypeStruct((shards, rows, width // shards), jnp.bfloat16),
        cost_estimate=pl.CostEstimate(
            flops=8 * rows * width, bytes_accessed=4 * rows * width, transcendentals=rows
        ),
    )(*parts, gain.reshape(1, width))


def finish_kernel(groups, place_ref, tokens_ref, *refs):
    pieces, hidden_ref = refs[:-1], refs[-1]
    width = tokens_ref.shape[1]
    planes = place_ref.shape[0]
    wide = width // planes
    for plane in range(planes):
        slot = place_ref[plane]
        cols = slice(plane * wide, (plane + 1) * wide)
        total = tokens_ref[:, cols].astype(jnp.float32)
        for first in range(0, len(pieces), groups):
            value = None
            base = 0
            for ref in pieces[first : first + groups]:
                count = ref.shape[0]
                part = ref[jnp.clip(slot - base, 0, count - 1)]
                value = part if value is None else jnp.where(slot >= base, part, value)
                base += count
            total += value.astype(jnp.float32)
        hidden_ref[:, cols] = total.astype(jnp.bfloat16)


def finish(place, tokens, pieces, groups):
    rows, width = tokens.shape

    def kernel(*refs):
        finish_kernel(groups, *refs)

    return pl.pallas_call(
        kernel,
        name="finish",
        out_shape=jax.ShapeDtypeStruct((rows, width), jnp.bfloat16),
        in_specs=[pl.BlockSpec(memory_space=pltpu.SMEM)]
        + [pl.BlockSpec(memory_space=pltpu.VMEM)] * (1 + len(pieces)),
        cost_estimate=pl.CostEstimate(
            flops=8 * rows * width, bytes_accessed=6 * rows * width, transcendentals=0
        ),
    )(place, tokens, *pieces)


def score_kernel(slots_ref, weight_ref, last_ref, gained_ref, *refs):
    rows, out_ref = refs[:-1], refs[-1]
    planes = last_ref.shape[0]
    count = rows[0].shape[0]
    at = lax.broadcasted_iota(jnp.int32, (planes, count), 0)
    slot = jnp.zeros((planes, count), jnp.int32)
    for plane in range(planes):
        slot = jnp.where(at == plane, slots_ref[plane], slot)
    block = lax.broadcasted_iota(jnp.int32, (planes, count), 1)
    chosen = jnp.where(slot == block, 1.0, 0.0).astype(jnp.bfloat16)
    total = last_ref[...].astype(jnp.float32)
    for ref in rows:
        total += jnp.dot(chosen, ref[...], preferred_element_type=jnp.float32)
    total = total.astype(jnp.bfloat16).astype(jnp.float32)

    def summed(values):
        return jnp.sum(jnp.sum(values, axis=1, keepdims=True), axis=0, keepdims=True)

    width = last_ref.shape[0] * last_ref.shape[1]
    score = summed(total * gained_ref[...]) * lax.rsqrt(summed(total * total) / width + 1e-06)
    lane = lax.broadcasted_iota(jnp.int32, out_ref.shape, 1)
    out_ref[...] = jnp.where(lane == 0, score, weight_ref[0])


def score_rows(place, pair_weight, last, gained, ahead, total_seqs):
    return pl.pallas_call(
        score_kernel,
        name="score",
        out_shape=jax.ShapeDtypeStruct((total_seqs, 128), jnp.float32),
        in_specs=[pl.BlockSpec(memory_space=pltpu.SMEM)] * 2
        + [pl.BlockSpec(memory_space=pltpu.VMEM)] * (2 + len(ahead)),
        cost_estimate=pl.CostEstimate(
            flops=8 * gained.size, bytes_accessed=16 * gained.size, transcendentals=1
        ),
    )(place, pair_weight, last, gained, *ahead)


def solution(mesh):
    fsdp_size = mesh.shape["fsdp"]
    dp_size = mesh.shape["dp"]
    planes = fsdp_size // 2
    ranks = dp_size
    query_heads = QUERY_HEADS // ranks
    key_value_heads = KEY_VALUE_HEADS // ranks
    query_cols = query_heads * HEAD_SIZE
    key_cols = key_value_heads * HEAD_SIZE

    def route(move):
        pairs = []
        for f in range(fsdp_size):
            for d in range(dp_size):
                target = move(f // 2, f % 2, d // 2, d % 2)
                if target is not None:
                    z, y, x, c = target
                    pairs.append((f * dp_size + d, (z * 2 + y) * dp_size + x * 2 + c))
        return pairs

    def send(array, move):
        return lax.ppermute(array, AXES, route(move))

    def to_y(z, y, x, c):
        return (z, 1 - y, x, c)

    def to_x(z, y, x, c):
        return (z, y, x ^ 1, c)

    def to_xy(z, y, x, c):
        return (z, 1 - y, x ^ 1, c)

    def to_core(z, y, x, c):
        return (z, y, x, 1 - c)

    def hop_y(z, y, x, c):
        return (z, 1 - y, x, 1 - c) if c != y else None

    def along(shift, holds):
        def move(z, y, x, c):
            return (z + shift, y, x, c) if holds(z) and 0 <= z + shift < planes else None

        return move

    def outward(step):
        def move(z, y, x, c):
            if z >= step - 1:
                return (z + 1, y, x, c) if z + 1 < planes else None
            if z + step <= planes:
                return (z - 1, y, x, c) if z >= 1 else None
            return None

        return move

    def whole(
        tokens,
        lengths,
        partner,
        pair_weight,
        norm_gain,
        qkv_weight,
        qkv_bias,
        out_weight,
        final_gain,
        value_head,
    ):
        f = lax.axis_index("fsdp")
        d = lax.axis_index("dp")
        z, y, x, c = f // 2, f % 2, d // 2, d % 2
        g = x * 2 + y
        sequence = tokens[0]
        length = lengths[0]
        length_rows, _ = sequence.shape

        def group_slices(array, group, dim):
            return jnp.concatenate(
                [
                    lax.dynamic_slice_in_dim(array, group * query_cols, query_cols, dim),
                    lax.dynamic_slice_in_dim(
                        array, QUERY_FEATURES + group * key_cols, key_cols, dim
                    ),
                    lax.dynamic_slice_in_dim(
                        array, QUERY_FEATURES + KEY_FEATURES + group * key_cols, key_cols, dim
                    ),
                ],
                axis=dim,
            )

        def spread(own, gate=None):
            found = [(z, own, 0)]
            up = down = merged = own
            for step in range(1, planes):
                low, high = z >= step, z + step < planes
                below = jnp.where(low, z - step, -1)
                above = jnp.where(high, z + step, -1)
                if 2 * step <= planes:
                    go_up = along(1, lambda p, step=step: p >= step - 1)
                    go_down = along(-1, lambda p, step=step: p + step <= planes)
                    up = send(up, go_up)
                    down = send(down, go_down)
                    if step == 1 and gate is not None:
                        up, down, _ = lax.optimization_barrier((up, down, gate))
                    if 2 * step < planes:
                        found += [(below, up, step), (above, down, step)]
                        continue
                    merged = jnp.where(low, up, down)
                else:
                    merged = send(merged, outward(step))
                found.append((jnp.where(low, below, above), merged, step))
            return found

        near = c == y

        cut = group_slices(qkv_weight, jnp.where(near, g, g ^ 1), 1)
        chain = spread(cut)
        qkv_blocks = [
            (plane, jnp.where(near, block, send(block, hop_y)))
            for plane, block, _ in chain
        ]
        others = [send(own, to_core) for _, own in qkv_blocks]

        by_y = send(sequence, to_y)
        by_x = send(sequence, to_x)
        far = send(by_y, to_x)
        normed = normalise([sequence, by_y, by_x, far], norm_gain, fsdp_size)
        near_lengths = [send(lengths, to_y), send(lengths, to_x), send(lengths, to_xy)]
        group_lengths = [lengths, *near_lengths]
        row_places = [
            j * length_rows + group_length - 1 for j, group_length in enumerate(group_lengths)
        ]
        normed, near_lengths, row_places = lax.optimization_barrier(
            (normed, near_lengths, row_places)
        )
        group_lengths = [lengths, *near_lengths]
        acc = None
        for (plane, own), other in zip(qkv_blocks, others):
            for core, weights in ((c, own), (1 - c, other)):
                part = jnp.dot(
                    lax.dynamic_index_in_dim(normed, jnp.maximum(plane, 0) * 2 + core, 0, False),
                    weights,
                    preferred_element_type=jnp.float32,
                )
                acc = part if acc is None else acc + part

        attn = attend(
            acc,
            group_slices(qkv_bias, g, 0),
            rotary_tables(length_rows),
            group_lengths,
            query_heads,
            length_rows,
        )

        cut = lax.dynamic_slice_in_dim(
            out_weight.T, jnp.where(near, g, g ^ 1) * query_cols, query_cols, 1
        )
        hopped = send(cut, hop_y)
        kept = jnp.where(near, cut, hopped)
        out_blocks = spread(kept, attn)
        groups = [[], [], []]
        for index, (_, own, step) in enumerate(out_blocks):
            other = send(own, to_core)
            weights = jnp.where(
                c == 0,
                jnp.concatenate([own, other], axis=0),
                jnp.concatenate([other, own], axis=0),
            )
            part = lax.dot_general(
                attn, weights, (((1,), (1,)), ((), ())), preferred_element_type=jnp.float32
            ).astype(jnp.bfloat16)
            at = 0 if 2 * step < planes else 1
            groups[2 if index == len(out_blocks) - 1 else at].append(part)
        groups = [group for group in groups if group]
        parts = [part for group in groups for part in group]
        ahead = []
        for j, move in enumerate((None, to_y, to_x, to_xy)):
            at = row_places[j][0]
            rows = [lax.dynamic_slice_in_dim(part, at, 1, 0) for part in parts]
            chosen = jnp.concatenate(rows, axis=0)
            ahead.append(chosen if move is None else send(chosen, move))
        pieces = []
        for j, move in enumerate((None, to_y, to_x, to_xy)):
            for group in groups:
                rows = slice(j * length_rows, (j + 1) * length_rows)
                piece = jnp.stack([part[rows] for part in group])
                pieces.append(piece if move is None else send(piece, move))
        counted = []
        for group in (0, 1, 2):
            for index, (plane, _, step) in enumerate(out_blocks):
                at = 0 if 2 * step < planes else 1
                if group == (2 if index == len(out_blocks) - 1 else at):
                    counted.append(plane)
        slots = [
            sum(b * (plane == p).astype(jnp.int32) for b, plane in enumerate(counted))
            for p in range(planes)
        ]
        place = jnp.stack(slots).astype(jnp.int32)
        hidden = finish(place, sequence, pieces, len(groups))
        last = lax.dynamic_slice_in_dim(sequence, length - 1, 1, 0).reshape(planes, -1)
        gained = (final_gain * value_head).reshape(planes, -1)
        total_seqs = fsdp_size * dp_size
        both = score_rows(place, pair_weight, last, gained, ahead, total_seqs)

        index_all = jnp.arange(total_seqs, dtype=jnp.int32)
        mine = f * dp_size + d
        gathered = lax.all_to_all(both, AXES, 0, 0, tiled=True)
        everyone = gathered[:, 0]
        weights_all = gathered[:, 1]
        matches = partner[:, None] == index_all[None, :]
        others_all = jnp.sum(jnp.where(matches, everyone[None, :], jnp.float32(0.0)), axis=1)
        margins_all = jnp.where(index_all < partner, everyone - others_all, others_all - everyone)
        margin = jnp.sum(jnp.where(index_all == mine, margins_all, 0.0))
        loss = jnp.sum(weights_all * jax.nn.softplus(-margins_all)) / total_seqs
        return (hidden[None], margin.reshape(1), loss)


    return jax.shard_map(
        whole,
        mesh=mesh,
        in_specs=(
            P(("fsdp", "dp"), None, None),
            P(("fsdp", "dp")),
            P(),
            P(("fsdp", "dp")),
            P(),
            P("fsdp", None),
            P(),
            P(None, "fsdp"),
            P(),
            P(),
        ),
        out_specs=(P(("fsdp", "dp"), None, None), P(("fsdp", "dp")), P()),
        check_vma=False,
    )
```

```python
import jax
import jax.numpy as jnp
from jax import lax
from jax.experimental import pallas as pl
from jax.experimental.pallas import tpu as pltpu
from jax.sharding import PartitionSpec as P


QUERY_HEADS = 28
KEY_VALUE_HEADS = 4
HEAD_SIZE = 128
QUERY_FEATURES = 3584
KEY_FEATURES = 512
AXES = ("fsdp", "dp")


def rms_scale(value_rows, gain):
    return (
        value_rows
        * lax.rsqrt(jnp.mean(value_rows * value_rows, axis=-1, keepdims=True) + 1e-06)
        * gain
    )


def rotary_tables(length_rows):
    half = HEAD_SIZE // 2
    positions = jnp.arange(length_rows, dtype=jnp.float32)
    freqs = jnp.exp(
        -(2.0 * jnp.arange(half, dtype=jnp.float32) / HEAD_SIZE) * jnp.log(jnp.float32(1000000.0))
    )
    angles = positions[:, None] * freqs[None, :]
    cosine = jnp.cos(angles)
    sine = jnp.sin(angles)
    return (
        jnp.concatenate([cosine, cosine], axis=-1),
        jnp.concatenate([-sine, sine], axis=-1),
    )


def attention_kernel(
    query_heads, lengths_ref, acc_ref, bias_ref, cos_ref, sin_ref, out_ref
):
    length = lengths_ref[pl.program_id(0)]
    rows = acc_ref.shape[0]
    cosine = cos_ref[...]
    sine = sin_ref[...]

    def head(index):
        cols = pl.ds(index * HEAD_SIZE, HEAD_SIZE)
        return acc_ref[:, cols] + bias_ref[:, cols]

    def rotate(values):
        return (
            values * cosine + pltpu.roll(values, HEAD_SIZE // 2, 1) * sine
        ).astype(jnp.bfloat16)

    key_rows = rotate(head(query_heads))
    value_rows = head(query_heads + 1).astype(jnp.bfloat16)
    row = lax.broadcasted_iota(jnp.int32, (rows, rows), 0)
    col = lax.broadcasted_iota(jnp.int32, (rows, rows), 1)
    allowed = (col <= row) & (col < length)
    scale = 1.0 / jnp.sqrt(jnp.float32(HEAD_SIZE))
    scores = []
    for index in range(query_heads):
        raw = lax.dot_general(
            rotate(head(index)),
            key_rows,
            (((1,), (1,)), ((), ())),
            preferred_element_type=jnp.float32,
        )
        scores.append(jnp.where(allowed, raw * scale, jnp.float32(-1e30)))
    probs = []
    for score in scores:
        expd = jnp.exp(score - jnp.max(score, axis=-1, keepdims=True))
        inverse = 1.0 / jnp.sum(expd, axis=-1, keepdims=True)
        probs.append((expd * inverse).astype(jnp.bfloat16))
    for index, prob in enumerate(probs):
        mixed = jnp.dot(prob, value_rows, preferred_element_type=jnp.float32)
        out_ref[:, pl.ds(index * HEAD_SIZE, HEAD_SIZE)] = mixed.astype(jnp.bfloat16)


def attend(acc, bias_cols, tables, group_lengths, query_heads, length_rows):
    total_rows, width = acc.shape
    seq_count = total_rows // length_rows
    query_cols = query_heads * HEAD_SIZE

    def kernel(*refs):
        attention_kernel(query_heads, *refs)

    return pl.pallas_call(
        kernel,
        name="attention",
        out_shape=jax.ShapeDtypeStruct((total_rows, query_cols), jnp.bfloat16),
        grid_spec=pltpu.PrefetchScalarGridSpec(
            num_scalar_prefetch=1,
            grid=(seq_count,),
            in_specs=[
                pl.BlockSpec((length_rows, width), lambda i, *lengths: (i, 0)),
                pl.BlockSpec((1, width), lambda i, *lengths: (0, 0)),
                pl.BlockSpec((length_rows, HEAD_SIZE), lambda i, *lengths: (0, 0)),
                pl.BlockSpec((length_rows, HEAD_SIZE), lambda i, *lengths: (0, 0)),
            ],
            out_specs=pl.BlockSpec((length_rows, query_cols), lambda i, *lengths: (i, 0)),
        ),
        cost_estimate=pl.CostEstimate(
            flops=32 * seq_count * query_heads * length_rows * length_rows * HEAD_SIZE,
            bytes_accessed=acc.size * 4 + total_rows * query_cols * 2,
            transcendentals=seq_count * query_heads * length_rows * length_rows,
        ),
    )(group_lengths, acc, bias_cols.reshape(1, width), *tables)


def norm_kernel(own_ref, by_y_ref, by_x_ref, far_ref, gain_ref, out_ref):
    shards, _, shard_rows = out_ref.shape
    step = own_ref.shape[0] // 2
    base = 0
    for source in (own_ref, by_y_ref, by_x_ref, far_ref):

        def body(i, carry, source=source, base=base):
            start = pl.multiple_of(i * step, step)
            values = source[pl.ds(start, step), :].astype(jnp.float32)
            normed = rms_scale(values, gain_ref[...]).astype(jnp.bfloat16)
            target = pl.ds(pl.multiple_of(base + i * step, step), step)
            for s in range(shards):
                out_ref[s, target, :] = normed[:, s * shard_rows : (s + 1) * shard_rows]
            return carry

        lax.fori_loop(0, source.shape[0] // step, body, 0)
        base += source.shape[0]


def normalise(parts, gain, shards):
    rows = sum(part.shape[0] for part in parts)
    width = gain.shape[0]
    return pl.pallas_call(
        norm_kernel,
        name="normalise",
        out_shape=jax.ShapeDtypeStruct((shards, rows, width // shards), jnp.bfloat16),
        cost_estimate=pl.CostEstimate(
            flops=8 * rows * width, bytes_accessed=4 * rows * width, transcendentals=rows
        ),
    )(*parts, gain.reshape(1, width))


def finish_kernel(groups, place_ref, tokens_ref, *refs):
    pieces, hidden_ref = refs[:-1], refs[-1]
    width = tokens_ref.shape[1]
    planes = place_ref.shape[0]
    wide = width // planes
    for plane in range(planes):
        slot = place_ref[plane]
        cols = slice(plane * wide, (plane + 1) * wide)
        total = tokens_ref[:, cols].astype(jnp.float32)
        for first in range(0, len(pieces), groups):
            value = None
            base = 0
            for ref in pieces[first : first + groups]:
                count = ref.shape[0]
                part = ref[jnp.clip(slot - base, 0, count - 1)]
                value = part if value is None else jnp.where(slot >= base, part, value)
                base += count
            total += value.astype(jnp.float32)
        hidden_ref[:, cols] = total.astype(jnp.bfloat16)


def finish(place, tokens, pieces, groups):
    rows, width = tokens.shape

    def kernel(*refs):
        finish_kernel(groups, *refs)

    return pl.pallas_call(
        kernel,
        name="finish",
        out_shape=jax.ShapeDtypeStruct((rows, width), jnp.bfloat16),
        in_specs=[pl.BlockSpec(memory_space=pltpu.SMEM)]
        + [pl.BlockSpec(memory_space=pltpu.VMEM)] * (1 + len(pieces)),
        cost_estimate=pl.CostEstimate(
            flops=8 * rows * width, bytes_accessed=6 * rows * width, transcendentals=0
        ),
    )(place, tokens, *pieces)


def score_kernel(slots_ref, weight_ref, last_ref, gained_ref, *refs):
    rows, out_ref = refs[:-1], refs[-1]
    planes = last_ref.shape[0]
    count = rows[0].shape[0]
    at = lax.broadcasted_iota(jnp.int32, (planes, count), 0)
    slot = jnp.zeros((planes, count), jnp.int32)
    for plane in range(planes):
        slot = jnp.where(at == plane, slots_ref[plane], slot)
    block = lax.broadcasted_iota(jnp.int32, (planes, count), 1)
    chosen = jnp.where(slot == block, 1.0, 0.0).astype(jnp.bfloat16)
    total = last_ref[...].astype(jnp.float32)
    for ref in rows:
        total += jnp.dot(chosen, ref[...], preferred_element_type=jnp.float32)
    total = total.astype(jnp.bfloat16).astype(jnp.float32)

    def summed(values):
        return jnp.sum(jnp.sum(values, axis=1, keepdims=True), axis=0, keepdims=True)

    width = last_ref.shape[0] * last_ref.shape[1]
    score = summed(total * gained_ref[...]) * lax.rsqrt(summed(total * total) / width + 1e-06)
    lane = lax.broadcasted_iota(jnp.int32, out_ref.shape, 1)
    out_ref[...] = jnp.where(lane == 0, score, weight_ref[0])


def score_rows(place, pair_weight, last, gained, ahead, total_seqs):
    return pl.pallas_call(
        score_kernel,
        name="score",
        out_shape=jax.ShapeDtypeStruct((total_seqs, 128), jnp.float32),
        in_specs=[pl.BlockSpec(memory_space=pltpu.SMEM)] * 2
        + [pl.BlockSpec(memory_space=pltpu.VMEM)] * (2 + len(ahead)),
        cost_estimate=pl.CostEstimate(
            flops=8 * gained.size, bytes_accessed=16 * gained.size, transcendentals=1
        ),
    )(place, pair_weight, last, gained, *ahead)


def solution(mesh):
    fsdp_size = mesh.shape["fsdp"]
    dp_size = mesh.shape["dp"]
    planes = fsdp_size // 2
    ranks = dp_size
    query_heads = QUERY_HEADS // ranks
    key_value_heads = KEY_VALUE_HEADS // ranks
    query_cols = query_heads * HEAD_SIZE
    key_cols = key_value_heads * HEAD_SIZE

    def route(move):
        pairs = []
        for f in range(fsdp_size):
            for d in range(dp_size):
                target = move(f // 2, f % 2, d // 2, d % 2)
                if target is not None:
                    z, y, x, c = target
                    pairs.append((f * dp_size + d, (z * 2 + y) * dp_size + x * 2 + c))
        return pairs

    def send(array, move):
        return lax.ppermute(array, AXES, route(move))

    def to_y(z, y, x, c):
        return (z, 1 - y, x, c)

    def to_x(z, y, x, c):
        return (z, y, x ^ 1, c)

    def to_xy(z, y, x, c):
        return (z, 1 - y, x ^ 1, c)

    def to_core(z, y, x, c):
        return (z, y, x, 1 - c)

    def hop_y(z, y, x, c):
        return (z, 1 - y, x, 1 - c) if c != y else None

    def along(shift, holds):
        def move(z, y, x, c):
            return (z + shift, y, x, c) if holds(z) and 0 <= z + shift < planes else None

        return move

    def outward(step):
        def move(z, y, x, c):
            if z >= step - 1:
                return (z + 1, y, x, c) if z + 1 < planes else None
            if z + step <= planes:
                return (z - 1, y, x, c) if z >= 1 else None
            return None

        return move

    def whole(
        tokens,
        lengths,
        partner,
        pair_weight,
        norm_gain,
        qkv_weight,
        qkv_bias,
        out_weight,
        final_gain,
        value_head,
    ):
        f = lax.axis_index("fsdp")
        d = lax.axis_index("dp")
        z, y, x, c = f // 2, f % 2, d // 2, d % 2
        g = x * 2 + y
        sequence = tokens[0]
        length = lengths[0]
        length_rows, _ = sequence.shape

        def group_slices(array, group, dim):
            return jnp.concatenate(
                [
                    lax.dynamic_slice_in_dim(array, group * query_cols, query_cols, dim),
                    lax.dynamic_slice_in_dim(
                        array, QUERY_FEATURES + group * key_cols, key_cols, dim
                    ),
                    lax.dynamic_slice_in_dim(
                        array, QUERY_FEATURES + KEY_FEATURES + group * key_cols, key_cols, dim
                    ),
                ],
                axis=dim,
            )

        def spread(own, gate=None):
            found = [(z, own, 0)]
            up = down = merged = own
            for step in range(1, planes):
                low, high = z >= step, z + step < planes
                below = jnp.where(low, z - step, -1)
                above = jnp.where(high, z + step, -1)
                if 2 * step <= planes:
                    go_up = along(1, lambda p, step=step: p >= step - 1)
                    go_down = along(-1, lambda p, step=step: p + step <= planes)
                    up = send(up, go_up)
                    down = send(down, go_down)
                    if step == 1 and gate is not None:
                        up, down, _ = lax.optimization_barrier((up, down, gate))
                    if 2 * step < planes:
                        found += [(below, up, step), (above, down, step)]
                        continue
                    merged = jnp.where(low, up, down)
                else:
                    merged = send(merged, outward(step))
                found.append((jnp.where(low, below, above), merged, step))
            return found

        near = c == y

        cut = group_slices(qkv_weight, jnp.where(near, g, g ^ 1), 1)
        chain = spread(cut)
        qkv_blocks = [
            (plane, jnp.where(near, block, send(block, hop_y)))
            for plane, block, _ in chain
        ]
        others = [send(own, to_core) for _, own in qkv_blocks]

        by_y = send(sequence, to_y)
        by_x = send(sequence, to_x)
        far = send(by_y, to_x)
        normed = normalise([sequence, by_y, by_x, far], norm_gain, fsdp_size)
        near_lengths = [send(lengths, to_y), send(lengths, to_x), send(lengths, to_xy)]
        group_lengths = [lengths, *near_lengths]
        row_places = [
            j * length_rows + group_length - 1 for j, group_length in enumerate(group_lengths)
        ]
        normed, group_lengths, row_places = lax.optimization_barrier(
            (normed, jnp.stack(group_lengths)[:, 0], row_places)
        )
        acc = None
        for (plane, own), other in zip(qkv_blocks, others):
            for core, weights in ((c, own), (1 - c, other)):
                part = jnp.dot(
                    lax.dynamic_index_in_dim(normed, jnp.maximum(plane, 0) * 2 + core, 0, False),
                    weights,
                    preferred_element_type=jnp.float32,
                )
                acc = part if acc is None else acc + part

        attn = attend(
            acc,
            group_slices(qkv_bias, g, 0),
            rotary_tables(length_rows),
            group_lengths,
            query_heads,
            length_rows,
        )

        cut = lax.dynamic_slice_in_dim(
            out_weight.T, jnp.where(near, g, g ^ 1) * query_cols, query_cols, 1
        )
        hopped = send(cut, hop_y)
        kept = jnp.where(near, cut, hopped)
        out_blocks = spread(kept, attn)
        groups = [[], [], []]
        for index, (_, own, step) in enumerate(out_blocks):
            other = send(own, to_core)
            weights = jnp.where(
                c == 0,
                jnp.concatenate([own, other], axis=0),
                jnp.concatenate([other, own], axis=0),
            )
            part = lax.dot_general(
                attn, weights, (((1,), (1,)), ((), ())), preferred_element_type=jnp.float32
            ).astype(jnp.bfloat16)
            at = 0 if 2 * step < planes else 1
            groups[2 if index == len(out_blocks) - 1 else at].append(part)
        groups = [group for group in groups if group]
        parts = [part for group in groups for part in group]
        ahead = []
        for j, move in enumerate((None, to_y, to_x, to_xy)):
            at = row_places[j][0]
            rows = [lax.dynamic_slice_in_dim(part, at, 1, 0) for part in parts]
            chosen = jnp.concatenate(rows, axis=0)
            ahead.append(chosen if move is None else send(chosen, move))
        pieces = []
        for j, move in enumerate((None, to_y, to_x, to_xy)):
            for group in groups:
                rows = slice(j * length_rows, (j + 1) * length_rows)
                piece = jnp.stack([part[rows] for part in group])
                pieces.append(piece if move is None else send(piece, move))
        counted = []
        for group in (0, 1, 2):
            for index, (plane, _, step) in enumerate(out_blocks):
                at = 0 if 2 * step < planes else 1
                if group == (2 if index == len(out_blocks) - 1 else at):
                    counted.append(plane)
        slots = [
            sum(b * (plane == p).astype(jnp.int32) for b, plane in enumerate(counted))
            for p in range(planes)
        ]
        place = jnp.stack(slots).astype(jnp.int32)
        hidden = finish(place, sequence, pieces, len(groups))
        last = lax.dynamic_slice_in_dim(sequence, length - 1, 1, 0).reshape(planes, -1)
        gained = (final_gain * value_head).reshape(planes, -1)
        total_seqs = fsdp_size * dp_size
        both = score_rows(place, pair_weight, last, gained, ahead, total_seqs)

        index_all = jnp.arange(total_seqs, dtype=jnp.int32)
        mine = f * dp_size + d
        gathered = lax.all_to_all(both, AXES, 0, 0, tiled=True)
        everyone = gathered[:, 0]
        weights_all = gathered[:, 1]
        matches = partner[:, None] == index_all[None, :]
        others_all = jnp.sum(jnp.where(matches, everyone[None, :], jnp.float32(0.0)), axis=1)
        margins_all = jnp.where(index_all < partner, everyone - others_all, others_all - everyone)
        margin = jnp.sum(jnp.where(index_all == mine, margins_all, 0.0))
        loss = jnp.sum(weights_all * jax.nn.softplus(-margins_all)) / total_seqs
        return (hidden[None], margin.reshape(1), loss)


    return jax.shard_map(
        whole,
        mesh=mesh,
        in_specs=(
            P(("fsdp", "dp"), None, None),
            P(("fsdp", "dp")),
            P(),
            P(("fsdp", "dp")),
            P(),
            P("fsdp", None),
            P(),
            P(None, "fsdp"),
            P(),
            P(),
        ),
        out_specs=(P(("fsdp", "dp"), None, None), P(("fsdp", "dp")), P()),
        check_vma=False,
    )
```
